32 devices in a mesh: dp: 2 (over x), tp: 4 (over z), ep: 4 (over y, core).
Axes of the slice: x: 2, y: 2, z: 4, core: 2. Of those that a mesh axis runs over, the one named last changes fastest.
Arguments:
- tokens: bfloat16 [4096, 1536], P(('dp', 'ep', 'tp')), parts along dimension 0
- expert_ids: int32 [4096, 6], P(('dp', 'ep', 'tp')), parts along dimension 0
- gates: float32 [4096, 6], P(('dp', 'ep', 'tp')), parts along dimension 0
- slots: int32 [4096, 6], P(('dp', 'ep', 'tp')), parts along dimension 0
- shared_w1: bfloat16 [1536, 1024], P(None, 'tp')
- shared_w3: bfloat16 [1536, 1024], P(None, 'tp')
- shared_w2: bfloat16 [1024, 1536], P('tp')
- expert_w1: bfloat16 [64, 1536, 512], P('ep')
- expert_w3: bfloat16 [64, 1536, 512], P('ep')
- expert_w2: bfloat16 [64, 512, 1536], P('ep')
Outputs:
- output: bfloat16 [4096, 1536], P(('dp', 'ep', 'tp')), parts along dimension 0
There are 2 independent parts. The reference program is written for one: setup_inputs(seed, part) draws one part's arguments, and reference() takes and returns one part's arrays. A program takes and returns all parts, laid end to end along the dimension named above; an argument that names none is the same for every part.
All inputs are finite; a program needn't handle non-finite values.
Results may differ from the reference program's by a relative error of at most 0.001.
Values are sent between devices in bfloat16 or wider.
A program may use at most 1 GiB of HBM per device.

```python
import jax
import jax.numpy as jnp
from jax import lax

D_MODEL = 1536
FF_EXPERT = 512
FF_SHARED = 1024
EXPERTS = 64
TOP_K = 6
TOKENS_DEV = 128
EP_SIZE = 4
TP_SIZE = 4
CAPACITY = 24

N_SOURCES = EP_SIZE * TP_SIZE
N_TOKENS = N_SOURCES * TOKENS_DEV


def draw_routing(route_key):
    key_hot, key_score = jax.random.split(route_key)
    hot_ids = jax.random.randint(key_hot, (2,), 0, EXPERTS)
    expert_range = jnp.arange(EXPERTS, dtype=jnp.int32)
    scores = jax.random.randint(key_score, (N_TOKENS, EXPERTS), 0, 1024)
    favoured = jnp.any(expert_range[None, :] == hot_ids[:, None], axis=0).astype(jnp.int32) * 128
    row_pos = jnp.arange(N_TOKENS, dtype=jnp.int32) % TOKENS_DEV
    forced = ((row_pos[:, None] < CAPACITY) & (expert_range[None, :] == hot_ids[0])).astype(jnp.int32) * 4096
    keyed_scores = (scores + favoured[None, :] + forced) * EXPERTS + expert_range[None, :]
    top_vals, expert_ids = lax.top_k(keyed_scores, TOP_K)
    expert_ids = expert_ids.astype(jnp.int32)
    per_source = expert_ids.reshape(N_SOURCES, TOKENS_DEV * TOP_K)
    one_hot = (per_source[:, :, None] == expert_range[None, None, :]).astype(jnp.int32)
    position = jnp.sum(jnp.cumsum(one_hot, axis=1) * one_hot, axis=2) - 1
    slots = jnp.where(position < CAPACITY, position, -1)
    return expert_ids, slots.reshape(N_TOKENS, TOP_K).astype(jnp.int32)


def normal_weights(weight_key, shape, fan_in):
    return (jax.random.normal(weight_key, shape, jnp.float32) * fan_in ** -0.5).astype(jnp.bfloat16)


def setup_inputs(seed: int = 0, part: int = 0) -> dict:
    root_key = jax.random.key(seed)
    shared_key, base_key = jax.random.split(root_key)
    part_key = jax.random.fold_in(base_key, part)
    key_tok, key_route, key_gate = jax.random.split(part_key, 3)
    key_list = jax.random.split(shared_key, 6)
    tokens = jax.random.normal(key_tok, (N_TOKENS, D_MODEL), jnp.float32).astype(jnp.bfloat16)
    expert_ids, slots = draw_routing(key_route)
    gates = jax.random.uniform(key_gate, (N_TOKENS, TOP_K), jnp.float32, 0.5, 1.0)
    return {
        "tokens": tokens,
        "expert_ids": expert_ids,
        "gates": gates,
        "slots": slots,
        "shared_w1": normal_weights(key_list[0], (D_MODEL, FF_SHARED), D_MODEL),
        "shared_w3": normal_weights(key_list[1], (D_MODEL, FF_SHARED), D_MODEL),
        "shared_w2": normal_weights(key_list[2], (FF_SHARED, D_MODEL), FF_SHARED),
        "expert_w1": normal_weights(key_list[3], (EXPERTS, D_MODEL, FF_EXPERT), D_MODEL),
        "expert_w3": normal_weights(key_list[4], (EXPERTS, D_MODEL, FF_EXPERT), D_MODEL),
        "expert_w2": normal_weights(key_list[5], (EXPERTS, FF_EXPERT, D_MODEL), FF_EXPERT),
    }


def swiglu_rows(token_rows, w_gate, w_up, w_down):
    gate_pre = jnp.dot(token_rows, w_gate, preferred_element_type=jnp.float32)
    up_pre = jnp.dot(token_rows, w_up, preferred_element_type=jnp.float32)
    hidden = (jax.nn.silu(gate_pre) * up_pre).astype(jnp.bfloat16)
    return jnp.dot(hidden, w_down, preferred_element_type=jnp.float32)


def reference(tokens, expert_ids, gates, slots, shared_w1, shared_w3, shared_w2, expert_w1, expert_w3, expert_w2):
    token_blocks = tokens.reshape(N_SOURCES, TOKENS_DEV, D_MODEL)

    def shared_block(block_rows):
        return swiglu_rows(block_rows, shared_w1, shared_w3, shared_w2)

    shared_out = lax.map(shared_block, token_blocks).reshape(N_TOKENS, D_MODEL)

    tok_ids = jnp.arange(N_TOKENS, dtype=jnp.int32)
    flat_tok = jnp.repeat(tok_ids, TOP_K)
    flat_src = flat_tok // TOKENS_DEV
    flat_exp = expert_ids.reshape(-1)
    flat_slot = jnp.where(slots.reshape(-1) >= 0, slots.reshape(-1), CAPACITY)
    inv_tok = jnp.full((EXPERTS, N_SOURCES, CAPACITY), N_TOKENS, jnp.int32).at[flat_exp, flat_src, flat_slot].set(flat_tok, mode="drop")
    inv_gate = jnp.zeros((EXPERTS, N_SOURCES, CAPACITY), jnp.float32).at[flat_exp, flat_src, flat_slot].set(gates.reshape(-1), mode="drop")

    def expert_step(accum_sum, step_inputs):
        rows_tok, rows_gate, w_gate, w_up, w_down = step_inputs
        tok_flat = rows_tok.reshape(-1)
        token_rows = jnp.take(tokens, tok_flat, axis=0, mode="fill", fill_value=0)
        expert_out = swiglu_rows(token_rows, w_gate, w_up, w_down).astype(jnp.bfloat16)
        weighted = rows_gate.reshape(-1)[:, None] * expert_out.astype(jnp.float32)
        return accum_sum.at[tok_flat].add(weighted, mode="drop"), None

    routed, unused_out = lax.scan(expert_step, jnp.zeros((N_TOKENS, D_MODEL), jnp.float32), (inv_tok, inv_gate, expert_w1, expert_w3, expert_w2))
    y_total = tokens.astype(jnp.float32) + shared_out + routed
    return y_total.astype(jnp.bfloat16)
```

```python
import functools

import jax
import jax.numpy as jnp
from jax import lax
from jax.experimental import pallas as pl
from jax.experimental.pallas import tpu as pltpu
from jax.sharding import PartitionSpec as P

MESH = pl.DeviceIdType.MESH
BF16, F32 = jnp.bfloat16, jnp.float32
RING = 24
Y_PARTS = 4


def dot(a, b):
    return jnp.dot(a, b, preferred_element_type=F32)


def glu(gate, up):
    return (gate * jax.nn.sigmoid(gate) * up).astype(BF16)


def moe_kernel(cap, n_col, ids_ref, gates_ref, slots_ref, tok, sw1, sw3, sw2, ew1, ew3, ew2, out_ref,
               route, x_all, xg, hid, ring, gt, rk, ws1, ws3, ws2, hs,
               racc, lacc, precv, ysend, yrecv, lrecv,
               own_sem, ring_sem, loc_sem, disp_s, disp_r, xo_s, xo_r, xf_s, xf_r,
               zup_s, zdn_s, z_r, xs_s, xs_r, ret_s, ret_r):
    n_tok, d_model = tok.shape
    n_exp = ew1.shape[0]
    top_k = ids_ref.shape[0]
    pair_rows = 2 * cap
    half_d = d_model // 2
    hid_w = sw1.shape[1] // 2
    col = d_model // n_col
    d, z, e = lax.axis_index("dp"), lax.axis_index("tp"), lax.axis_index("ep")
    c, y = lax.rem(e, 2), lax.div(e, 2)
    partner = {"ep": 2 * y + 1 - c}
    opp = {"ep": 2 * (1 - y) + c}
    x_peer = {"dp": 1 - d}
    up, down = {"tp": lax.rem(z + 1, 4)}, {"tp": lax.rem(z + 3, 4)}
    my_rows = pl.ds(pl.multiple_of(c * n_tok, n_tok), n_tok)

    def rdma(src, dst, send, recv, dev):
        return pltpu.make_async_remote_copy(src_ref=src, dst_ref=dst, send_sem=send, recv_sem=recv,
                                            device_id=dev, device_id_type=MESH)

    own = pltpu.make_async_copy(tok, x_all.at[0, my_rows, :], own_sem)
    own.start()

    def up_block(i, m):
        slot = lax.rem(2 * i + m, RING)
        return pltpu.make_async_copy((ew1, ew3)[m].at[i], ring.at[slot], ring_sem.at[slot, 0])

    def down_view(b):
        slot = lax.rem(2 * n_exp + lax.div(b, 3), RING)
        sub = lax.rem(b, 3)
        return slot, sub, ring.at[slot, pl.ds(pl.multiple_of(sub * 512, 512), 512), :]

    def down_block(b):
        slot, sub, view = down_view(b)
        k, i = lax.div(b, n_exp), lax.rem(b, n_exp)
        return pltpu.make_async_copy(ew2.at[i, :, pl.ds(pl.multiple_of(k * col, col), col)], view, ring_sem.at[slot, sub])

    for i in range(RING // 2):
        up_block(i, 0).start()
        up_block(i, 1).start()

    ids, slots = ids_ref[...], slots_ref[...]
    code = jnp.where(slots >= 0, ids * pair_rows + c * cap + slots, -100000)
    route[0, 0:top_k, my_rows] = code.astype(F32)
    route[0, 8:8 + top_k, my_rows] = gates_ref[...]

    barrier = pltpu.get_barrier_semaphore()

    def greet(dev):
        pl.semaphore_signal(barrier, inc=1, device_id=dev, device_id_type=MESH)

    greet(partner)
    greet(opp)
    greet(x_peer)

    @pl.when(z < 3)
    def _():
        greet(up)

    @pl.when(z > 0)
    def _():
        greet(down)

    pl.semaphore_wait(barrier, 4 + lax.rem(lax.div(z + 1, 2), 2))

    own.wait()
    my_route = route.at[0, :, my_rows]
    far_route = route.at[1, :, my_rows]
    rt_p = rdma(my_route, my_route, disp_s.at[0], disp_r.at[0], partner)
    rt_o = rdma(my_route, far_route, disp_s.at[1], disp_r.at[1], opp)
    rt_f = rdma(far_route, far_route, disp_s.at[2], disp_r.at[2], partner)
    x_p = rdma(x_all.at[0, my_rows, :], x_all.at[0, my_rows, :], disp_s.at[3], disp_r.at[3], partner)
    part = n_tok // Y_PARTS
    x_o, x_f = [], []
    for q in range(Y_PARTS):
        rows = pl.ds(pl.multiple_of(c * n_tok + q * part, part), part)
        x_o.append(rdma(x_all.at[0, rows, :], x_all.at[1, rows, :], xo_s.at[q], xo_r.at[q], opp))
        x_f.append(rdma(x_all.at[1, rows, :], x_all.at[1, rows, :], xf_s.at[q], xf_r.at[q], partner))
    rt_p.start()
    rt_o.start()
    x_p.start()
    for q in range(Y_PARTS):
        x_o[q].start()

    def span(i, n):
        return pl.ds(pl.multiple_of(i * n, n), n)

    def piece(j, m, half):
        if m == 2:
            return ws2.at[span(j, hid_w), span(half, half_d)]
        return (ws1, ws3)[m].at[span(half, half_d), span(j, hid_w)]

    def source(m, half):
        if m == 2:
            return sw2.at[span(y, hid_w), span(half, half_d)]
        return (sw1, sw3)[m].at[span(half, half_d), span(y, hid_w)]

    jn = lax.div(z, 2)
    jf = 1 - jn
    s_near = c + jn * (3 - 2 * c)
    s_far = c + jf * (3 - 2 * c)
    is_src = s_near == z

    def own_copy(m):
        if m == 2:
            return pltpu.make_async_copy(sw2.at[span(y, hid_w), :], ws2.at[span(jn, hid_w), :], loc_sem.at[m])
        return pltpu.make_async_copy((sw1, sw3)[m].at[:, span(y, hid_w)], (ws1, ws3)[m].at[:, span(jn, hid_w)], loc_sem.at[m])

    def send_up(src, j, m):
        return rdma(src, piece(j, m, d), zup_s.at[j, m], z_r.at[j, m], up)

    def send_down(src, j, m):
        return rdma(src, piece(j, m, d), zdn_s.at[j, m], z_r.at[j, m], down)

    def send_x(j, m):
        return rdma(piece(j, m, d), piece(j, m, d), xs_s.at[j, m], xs_r.at[j, m], x_peer)

    for m in range(3):
        @pl.when(jnp.logical_and(is_src, z < 3))
        def _():
            send_up(source(m, d), jn, m).start()

        @pl.when(jnp.logical_and(is_src, z > 0))
        def _():
            send_down(source(m, d), jn, m).start()

    for m in range(3):
        @pl.when(is_src)
        def _():
            own_copy(m).start()

    def forward(j, s, m):
        @pl.when(s != z)
        def _():
            send_up(piece(j, m, d), j, m).wait_recv()
            send_x(j, m).start()

        @pl.when(jnp.logical_and(z > s, z < 3))
        def _():
            send_up(piece(j, m, d), j, m).start()

        @pl.when(jnp.logical_and(z < s, z > 0))
        def _():
            send_down(piece(j, m, d), j, m).start()

    base = (e * (n_exp * pair_rows)).astype(F32)

    def place(p):
        group = 4
        n_rows = group * pair_rows

        def one(g, carry):
            first = (g * n_rows).astype(F32) + base
            rows = lax.broadcasted_iota(jnp.int32, (n_rows, 2 * n_tok), 0).astype(F32) + first
            hot = jnp.zeros((n_rows, 2 * n_tok), F32)
            for j in range(top_k):
                hot = jnp.where(route[p, j:j + 1, :] == rows, 1.0, hot)
            val = dot(hot.astype(BF16), x_all[p]).astype(BF16)
            for q in range(group):
                xg[g * group + q, p * pair_rows:(p + 1) * pair_rows, :] = val[q * pair_rows:(q + 1) * pair_rows]
            return carry

        lax.fori_loop(0, n_exp // group, one, 0)

    def gate_parts(p):
        n_rows = 256

        def one(g, carry):
            first = (g * n_rows).astype(F32) + base
            rows = lax.broadcasted_iota(jnp.int32, (n_rows, 2 * n_tok), 0).astype(F32) + first
            val = jnp.zeros((n_rows, 2 * n_tok), F32)
            for j in range(top_k):
                val = jnp.where(route[p, j:j + 1, :] == rows, route[p, 8 + j:9 + j, :], val)
            val = val.T
            g1 = val.astype(BF16)
            rest = val - g1.astype(F32)
            g2 = rest.astype(BF16)
            g3 = (rest - g2.astype(F32)).astype(BF16)
            cols = span(g, n_rows)
            gt[p, 0, :, cols] = g1
            gt[p, 1, :, cols] = g2
            gt[p, 2, :, cols] = g3
            return carry

        lax.fori_loop(0, n_exp * pair_rows // n_rows, one, 0)

    rt_p.wait_recv()
    x_p.wait_recv()
    place(0)
    gate_parts(0)
    rt_o.wait_recv()
    rt_f.start()
    for q in range(Y_PARTS):
        x_o[q].wait_recv()
        x_f[q].start()
        if q < 3:
            forward(jn, s_near, q)
    rt_f.wait_recv()
    gate_parts(1)
    for q in range(Y_PARTS):
        x_f[q].wait_recv()
    place(1)

    def expert(i, carry):
        slot = lax.rem(2 * i, RING)
        up_block(i, 0).wait()
        up_block(i, 1).wait()
        rows = xg[i]
        hid[i] = glu(dot(rows, ring[slot]), dot(rows, ring[slot + 1]))

        @pl.when(i < n_exp - RING // 2)
        def _():
            up_block(i + RING // 2, 0).start()
            up_block(i + RING // 2, 1).start()

        @pl.when(jnp.logical_and(i >= n_exp - RING // 2, i < RING // 2))
        def _():
            for q in range(6):
                down_block((i - (n_exp - RING // 2)) * 6 + q).start()

        return carry

    lax.fori_loop(0, 4, expert, 0)
    forward(jf, s_far, 0)
    lax.fori_loop(4, 10, expert, 0)
    forward(jf, s_far, 1)
    lax.fori_loop(10, n_exp, expert, 0)
    forward(jf, s_far, 2)

    for m in range(3):
        @pl.when(is_src)
        def _():
            own_copy(m).wait()

        @pl.when(s_near != z)
        def _():
            send_x(jn, m).wait_recv()

        send_x(jf, m).wait_recv()

    for p in range(2):
        hs[p] = glu(dot(x_all[p], ws1[...]), dot(x_all[p], ws3[...]))

    def combine(p, k):
        vals = rk[p]
        total = dot(hs[p], ws2[:, k * col:(k + 1) * col])
        for m in range(3):
            total += dot(gt[p, m], vals)
        return total

    ret_p, ret_l, ret_y = [], [], []
    for k in range(n_col):
        ret_p.append(rdma(racc.at[k, 1 - c], precv.at[k], ret_s.at[0, k], ret_r.at[0, k], partner))
        ret_l.append(rdma(lacc.at[k, 1 - c], lrecv.at[k], ret_s.at[1, k], ret_r.at[1, k], partner))
        ret_y.append(rdma(ysend.at[k], yrecv.at[k], ret_s.at[2, k], ret_r.at[2, k], opp))

        def down_rows(i, carry):
            b = k * n_exp + i
            down_block(b).wait()
            vals = dot(hid[i], down_view(b)[2][...]).astype(BF16)
            rows = span(i, pair_rows)
            rk[0, rows, :] = vals[0:pair_rows]
            rk[1, rows, :] = vals[pair_rows:]
            return carry

        lax.fori_loop(0, n_exp, down_rows, 0)
        total = combine(1, k)
        racc[k, 0] = total[0:n_tok]
        racc[k, 1] = total[n_tok:]
        ret_p[k].start()
        total = combine(0, k)
        lacc[k, 0] = total[0:n_tok]
        lacc[k, 1] = total[n_tok:]
        ret_p[k].wait_recv()
        ysend[k] = racc[k, c] + precv[k]
        ret_l[k].start()
        ret_y[k].start()

    for k in range(n_col):
        ret_l[k].wait_recv()
        ret_y[k].wait_recv()
        cols = slice(k * col, (k + 1) * col)
        out_ref[:, cols] = (x_all[0, my_rows, cols].astype(F32) + lacc[k, c] + lrecv[k] + yrecv[k]).astype(BF16)

    for copy in [rt_p, rt_o, rt_f, x_p] + x_o + x_f + ret_p + ret_l + ret_y:
        copy.wait_send()
    for m in range(3):
        for j, s in ((jn, s_near), (jf, s_far)):
            @pl.when(s != z)
            def _():
                send_x(j, m).wait_send()

            @pl.when(jnp.logical_and(z >= s, z < 3))
            def _():
                send_up(piece(j, m, d), j, m).wait_send()

            @pl.when(jnp.logical_and(z <= s, z > 0))
            def _():
                send_down(piece(j, m, d), j, m).wait_send()


def solution(mesh):
    ep_size = mesh.shape["ep"]
    row_spec = P(("dp", "ep", "tp"), None)
    expert_spec = P("ep", None, None)

    def local_layer(tokens, expert_ids, gates, slots, sw1, sw3, sw2, ew1, ew3, ew2):
        n_tok, d_model = tokens.shape
        top_k = expert_ids.shape[1]
        n_exp, _, ff = ew1.shape
        cap = 8 * max(1, -(-2 * n_tok * top_k // (8 * n_exp * ep_size)))
        pair_rows = 2 * cap
        n_col = d_model // ff
        hid_w = sw1.shape[1] // 2
        dma = pltpu.SemaphoreType.DMA
        vmem = pl.BlockSpec(memory_space=pltpu.VMEM)
        hbm = pl.BlockSpec(memory_space=pl.ANY)
        return pl.pallas_call(
            functools.partial(moe_kernel, cap, n_col),
            out_shape=jax.ShapeDtypeStruct((n_tok, d_model), BF16),
            in_specs=[vmem] * 3 + [hbm] * 7,
            out_specs=vmem,
            scratch_shapes=[
                pltpu.VMEM((2, 16, 2 * n_tok), F32),
                pltpu.VMEM((2, 2 * n_tok, d_model), BF16),
                pltpu.VMEM((n_exp, 2 * pair_rows, d_model), BF16),
                pltpu.VMEM((n_exp, 2 * pair_rows, ff), BF16),
                pltpu.VMEM((RING, d_model, ff), BF16),
                pltpu.VMEM((2, 3, 2 * n_tok, n_exp * pair_rows), BF16),
                pltpu.VMEM((2, n_exp * pair_rows, ff), BF16),
                pltpu.VMEM((d_model, 2 * hid_w), BF16),
                pltpu.VMEM((d_model, 2 * hid_w), BF16),
                pltpu.VMEM((2 * hid_w, d_model), BF16),
                pltpu.VMEM((2, 2 * n_tok, 2 * hid_w), BF16),
                pltpu.VMEM((n_col, 2, n_tok, ff), F32),
                pltpu.VMEM((n_col, 2, n_tok, ff), F32),
                pltpu.VMEM((n_col, n_tok, ff), F32),
                pltpu.VMEM((n_col, n_tok, ff), F32),
                pltpu.VMEM((n_col, n_tok, ff), F32),
                pltpu.VMEM((n_col, n_tok, ff), F32),
                dma, dma((RING, 3)), dma((3,)), dma((4,)), dma((4,)),
                dma((Y_PARTS,)), dma((Y_PARTS,)), dma((Y_PARTS,)), dma((Y_PARTS,)),
                dma((2, 3)), dma((2, 3)), dma((2, 3)), dma((2, 3)), dma((2, 3)),
                dma((3, n_col)), dma((3, n_col)),
            ],
            compiler_params=pltpu.CompilerParams(collective_id=0, has_side_effects=True, vmem_limit_bytes=67043328),
            name="moe_layer",
        )(expert_ids.T, gates.T, slots.T, tokens, sw1, sw3, sw2, ew1, ew3, ew2)

    return jax.shard_map(
        local_layer, mesh=mesh,
        in_specs=(row_spec, row_spec, row_spec, row_spec, P(None, "tp"), P(None, "tp"), P("tp", None), expert_spec, expert_spec, expert_spec),
        out_specs=row_spec, check_vma=False)
```

```python
import functools

import jax
import jax.numpy as jnp
from jax import lax
from jax.experimental import pallas as pl
from jax.experimental.pallas import tpu as pltpu
from jax.sharding import PartitionSpec as P

MESH = pl.DeviceIdType.MESH
BF16, F32 = jnp.bfloat16, jnp.float32
GROUP = 8
RING = 8
BLK = 512
COL = 256


def dot(a, b):
    return jnp.dot(a, b, preferred_element_type=F32)


def glu(gate, up):
    return (gate * jax.nn.sigmoid(gate) * up).astype(BF16)


def moe_kernel(cap, ids_ref, gates_ref, slots_ref, tok, sw1, sw3, sw2, ew1, ew3, ew2, out,
               route, x_all, hot, xg, acc_g, acc_u, hid, ring, gt, rk, ws1, ws3, ws2, hs,
               racc, lacc, precv, ysend, yrecv, lrecv, out_v,
               own_sem, ring_sem, loc_sem, rt_s, rt_r, xo_s, xo_r, xf_s, xf_r,
               zup_s, zdn_s, z_r, xs_s, xs_r, ret_s, ret_r, out_sem):
    n_tok, d_model = tok.shape
    n_exp, _, ff = ew1.shape
    top_k = ids_ref.shape[0]
    pair_rows = 2 * cap
    half_d = d_model // 2
    hid_w = sw1.shape[1] // 2
    n_blk = d_model // BLK
    n_col = d_model // COL
    n_up = 2 * n_exp * n_blk
    n_load = n_up + n_exp * n_blk
    d, z, e = lax.axis_index("dp"), lax.axis_index("tp"), lax.axis_index("ep")
    c, y = lax.rem(e, 2), lax.div(e, 2)
    partner = {"ep": 2 * y + 1 - c}
    opp = {"ep": 2 * (1 - y) + c}
    x_peer = {"dp": 1 - d}
    up, down = {"tp": lax.rem(z + 1, 4)}, {"tp": lax.rem(z + 3, 4)}

    def span(i, n):
        return pl.ds(pl.multiple_of(i * n, n), n)

    my_rows = span(c, n_tok)

    def rdma(src, dst, send, recv, dev):
        return pltpu.make_async_remote_copy(src_ref=src, dst_ref=dst, send_sem=send, recv_sem=recv,
                                            device_id=dev, device_id_type=MESH)

    own = pltpu.make_async_copy(tok, x_all.at[0, my_rows, :], own_sem)
    own.start()

    r = 1 - c
    jn = lax.div(z, 2)
    jf = 1 - jn
    s_near = r + jn * (3 - 2 * r)
    s_far = r + jf * (3 - 2 * r)
    is_src = s_near == z
    n_piece = 2 + n_blk
    half_h = hid_w // 2

    def own_copy(m):
        if m == 2:
            return pltpu.make_async_copy(sw2.at[span(y, hid_w), :], ws2.at[span(jn, hid_w), :], loc_sem.at[m])
        return pltpu.make_async_copy((sw1, sw3)[m].at[:, span(y, hid_w)], (ws1, ws3)[m].at[:, span(jn, hid_w)], loc_sem.at[m])

    @pl.when(is_src)
    def _():
        for m in range(3):
            own_copy(m).start()

    def load(n):
        if n < n_up:
            kc, i, m = n // (2 * n_exp), n // 2 % n_exp, n % 2
            src = (ew1, ew3)[m].at[i, pl.ds(kc * BLK, BLK), :]
        else:
            src = ew2.at[(n - n_up) % n_exp, :, pl.ds((n - n_up) // n_exp * BLK, BLK)]
        group = n // GROUP % RING
        return pltpu.make_async_copy(src, ring.at[group, n % GROUP], ring_sem.at[group])

    def start_group(g):
        if g * GROUP < n_load:
            for n in range(g * GROUP, (g + 1) * GROUP):
                load(n).start()

    def wait_group(g):
        pltpu.make_async_copy(ring.at[g % RING], ring.at[g % RING], ring_sem.at[g % RING]).wait()

    def block(n):
        return ring.at[n // GROUP % RING, n % GROUP]

    ids, slots = ids_ref[...], slots_ref[...]
    code = jnp.where(slots >= 0, ids * pair_rows + c * cap + slots, -100000)
    route[0, 0:top_k, my_rows] = code.astype(F32)
    route[0, 8:8 + top_k, my_rows] = gates_ref[...]

    barrier = pltpu.get_barrier_semaphore()

    def greet(dev):
        pl.semaphore_signal(barrier, inc=1, device_id=dev, device_id_type=MESH)

    greet(partner)
    greet(opp)
    greet(x_peer)

    @pl.when(z < 3)
    def _():
        greet(up)

    @pl.when(z > 0)
    def _():
        greet(down)

    own.wait()
    start_group(0)
    pl.semaphore_wait(barrier, 4 + lax.rem(lax.div(z + 1, 2), 2))
    my_route = route.at[0, :, my_rows]
    far_route = route.at[1, :, my_rows]
    rt_p = rdma(my_route, my_route, rt_s.at[0], rt_r.at[0], partner)
    rt_o = rdma(my_route, far_route, rt_s.at[1], rt_r.at[1], opp)
    rt_f = rdma(far_route, far_route, rt_s.at[2], rt_r.at[2], partner)
    mine = x_all.at[0, my_rows, :]
    x_p = rdma(mine, mine, rt_s.at[3], rt_r.at[3], partner)
    x_o, x_f = [], []
    for q in range(n_blk):
        cols = pl.ds(q * BLK, BLK)
        there = x_all.at[1, my_rows, cols]
        x_o.append(rdma(x_all.at[0, my_rows, cols], there, xo_s.at[q], xo_r.at[q], opp))
        x_f.append(rdma(there, there, xf_s.at[q], xf_r.at[q], partner))
    x_o[0].start()
    rt_o.start()
    x_p.start()
    rt_p.start()
    for q in range(1, n_blk):
        x_o[q].start()

    def piece(j, m, half):
        if m >= 2:
            return ws2.at[pl.ds(pl.multiple_of(j * hid_w + half * half_h, half_h), half_h), pl.ds((m - 2) * BLK, BLK)]
        return (ws1, ws3)[m].at[span(half, half_d), span(j, hid_w)]

    def send_up(j, m):
        return rdma(piece(j, m, d), piece(j, m, d), zup_s.at[j, m], z_r.at[j, m], up)

    def send_down(j, m):
        return rdma(piece(j, m, d), piece(j, m, d), zdn_s.at[j, m], z_r.at[j, m], down)

    def send_x(j, m):
        return rdma(piece(j, m, d), piece(j, m, d), xs_s.at[j, m], xs_r.at[j, m], x_peer)

    inner = lax.rem(lax.div(z + 1, 2), 2) == 1
    outer = jnp.logical_not(inner)
    in0, in1 = jnp.logical_and(inner, r == 0), jnp.logical_and(inner, r == 1)
    out0, out1 = jnp.logical_and(outer, r == 0), jnp.logical_and(outer, r == 1)

    def from_source(cond, pieces):
        for m in pieces:
            @pl.when(jnp.logical_and(cond, z < 3))
            def _():
                send_up(jn, m).start()

            @pl.when(jnp.logical_and(cond, z > 0))
            def _():
                send_down(jn, m).start()

    def forward(cond, far, *pieces):
        j, s = (jf, s_far) if far else (jn, s_near)

        @pl.when(cond)
        def _():
            for m in pieces:
                send_up(j, m).wait_recv()

                @pl.when(jnp.logical_and(z > s, z < 3))
                def _():
                    send_up(j, m).start()

                @pl.when(jnp.logical_and(z < s, z > 0))
                def _():
                    send_down(j, m).start()

                send_x(j, m).start()

    w2_pieces = tuple(range(2, n_piece))

    @pl.when(is_src)
    def _():
        for m in range(3):
            own_copy(m).wait()

    from_source(is_src, (0, 1))
    from_source(out0, w2_pieces)
    for g in range(1, RING):
        start_group(g)

    base = (e * (n_exp * pair_rows)).astype(F32)

    def matches(p, first, n_rows, value):
        rows = lax.broadcasted_iota(jnp.int32, (n_rows, 2 * n_tok), 0).astype(F32) + (base + first)
        val = jnp.zeros((n_rows, 2 * n_tok), F32)
        for j in range(top_k):
            val = jnp.where(route[p, j:j + 1, :] == rows, value(j), val)
        return val

    def mark_rows(p):
        for g in range(n_exp // 4):
            n_rows = 4 * pair_rows
            hot[p, g * n_rows:(g + 1) * n_rows, :] = matches(p, g * n_rows, n_rows, lambda j: 1.0).astype(BF16)

    def place(p, kc):
        cols = slice(kc * BLK, (kc + 1) * BLK)
        for g in range(n_exp // 4):
            n_rows = 4 * pair_rows
            val = dot(hot[p, g * n_rows:(g + 1) * n_rows, :], x_all[p, :, cols]).astype(BF16)
            for q in range(4):
                xg[g * 4 + q, p * pair_rows:(p + 1) * pair_rows, cols] = val[q * pair_rows:(q + 1) * pair_rows]

    def gate_part(p, g):
        n_rows = 256
        val = matches(p, g * n_rows, n_rows, lambda j: route[p, 8 + j:9 + j, :]).T
        g1 = val.astype(BF16)
        rest = val - g1.astype(F32)
        g2 = rest.astype(BF16)
        g3 = (rest - g2.astype(F32)).astype(BF16)
        cols = slice(g * n_rows, (g + 1) * n_rows)
        gt[p, 0, :, cols] = g1
        gt[p, 1, :, cols] = g2
        gt[p, 2, :, cols] = g3

    def experts(kc, i0, extras):
        cols = slice(kc * BLK, (kc + 1) * BLK)
        group = (kc * 2 * n_exp + 2 * i0) // GROUP
        wait_group(group)
        for i in range(i0, i0 + 4):
            n = kc * 2 * n_exp + 2 * i
            rows = xg[i, :, cols]
            g = dot(rows, block(n)[...])
            u = dot(rows, block(n + 1)[...])
            if kc > 0:
                g, u = acc_g[i] + g, acc_u[i] + u
            if kc < n_blk - 1:
                acc_g[i] = g
                acc_u[i] = u
            else:
                hid[i] = glu(g, u)
        for extra in extras:
            extra()
        start_group(group + RING)

    rt_p.wait_recv()
    x_p.wait_recv()
    mark_rows(0)
    place(0, 0)
    for g in range(n_exp * pair_rows // 256):
        gate_part(0, g)
    rt_o.wait_recv()
    rt_f.start()
    x_o[0].wait_recv()
    x_f[0].start()
    forward(in0, False, 0)
    forward(in1, True, 0)
    forward(out1, False, 0)
    for kc in range(1, n_blk):
        place(0, kc)
    rt_f.wait_recv()
    mark_rows(1)
    forward(in0, False, 1)
    forward(in1, True, 1)
    forward(out1, False, 1)
    n_gate = n_exp * pair_rows // 256

    plan = {
        (0, 4): [(in0, True, 0)],
        (0, 12): [(out1, True, 0)],
        (1, 0): [(in0, True, 1), (in0, False, 2)],
        (1, 4): [(out1, True, 1), (in1, True, 2)],
        (1, 8): [(out0, True, 0)],
        (1, 12): [(in0, False, 3, 4)],
        (2, 0): [(in0, True, 2)],
        (2, 4): [(out1, False, 2), (out1, True, 2)],
        (2, 8): [(out0, True, 1)],
        (2, 12): [(in0, True, 3, 4), (in1, True, 3, 4)],
    }
    for kc in range(n_blk):
        x_f[kc].wait_recv()
        place(1, kc)
        for i0 in range(0, n_exp, 4):
            part = kc * n_exp // 4 + i0 // 4
            experts(kc, i0, [functools.partial(gate_part, 1, part - 4)] if 4 <= part < 4 + n_gate else [])
            for args in plan.get((kc, i0), ()):
                forward(*args)
            if (kc, i0) == (0, 4):
                from_source(in1, (2,))
            if (kc, i0) == (1, 12):
                from_source(in1, w2_pieces[1:])
            if i0 == 4 and kc + 1 < n_blk:
                x_o[kc + 1].wait_recv()
                x_f[kc + 1].start()

    def need_near(m):
        @pl.when(s_near != z)
        def _():
            send_x(jn, m).wait_recv()

    def need_far(m):
        send_x(jf, m).wait_recv()

    def shared_hidden(p, j):
        cols = span(j, hid_w)
        hs[p, :, cols] = glu(dot(x_all[p], ws1[:, cols]), dot(x_all[p], ws3[:, cols]))

    def down_rows(kk):
        k, h = kk * COL // BLK, kk * COL % BLK
        if h == 0:
            for g in range(n_exp // GROUP):
                wait_group((n_up + k * n_exp) // GROUP + g)
        for i in range(n_exp):
            vals = dot(hid[i], block(n_up + k * n_exp + i)[:, h:h + COL]).astype(BF16)
            rows = pl.ds(i * pair_rows, pair_rows)
            rk[0, kk % 3, rows, :] = vals[0:pair_rows]
            rk[1, kk % 3, rows, :] = vals[pair_rows:]

    def combine(p, kk):
        vals = rk[p, kk % 3]
        total = dot(gt[p, 0], vals)
        for m in range(1, 3):
            total += dot(gt[p, m], vals)
        return total

    def shared_part(p, kk):
        return dot(hs[p], ws2[:, kk * COL:(kk + 1) * COL])

    ret_p, ret_l, ret_y = [], [], []
    for kk in range(n_col):
        ret_p.append(rdma(racc.at[kk, 1 - c], precv.at[kk], ret_s.at[0, kk], ret_r.at[0, kk], partner))
        ret_l.append(rdma(lacc.at[kk, 1 - c], lrecv.at[kk], ret_s.at[1, kk], ret_r.at[1, kk], partner))
        ret_y.append(rdma(ysend.at[kk], yrecv.at[kk], ret_s.at[2, kk], ret_r.at[2, kk], opp))

    def far_sum(kk):
        total = combine(1, kk)
        if kk == 0:
            racc[0, 0] = total[0:n_tok]
            racc[0, 1] = total[n_tok:]
            forward(out0, True, 2)
            need_near(0)
            need_near(1)
            shared_hidden(1, jn)
            need_far(0)
            need_far(1)
            shared_hidden(1, jf)
        if kk % 2 == 0:
            need_near(2 + kk // 2)
            need_far(2 + kk // 2)
        part = shared_part(1, kk)
        if kk == 0:
            racc[0, 0] = racc[0, 0] + part[0:n_tok]
            racc[0, 1] = racc[0, 1] + part[n_tok:]
        else:
            total += part
            racc[kk, 0] = total[0:n_tok]
            racc[kk, 1] = total[n_tok:]
        ret_p[kk].start()

    def near_sum(kk):
        total = combine(0, kk) + shared_part(0, kk)
        lacc[kk, 0] = total[0:n_tok]
        lacc[kk, 1] = total[n_tok:]
        ret_l[kk].start()

    down_rows(0)
    for kk in range(n_col):
        far_sum(kk)
        if kk > 0:
            near_sum(kk - 1)
        if kk + 1 < n_col:
            down_rows(kk + 1)
        ret_p[kk].wait_recv()
        ysend[kk] = racc[kk, c] + precv[kk]
        ret_y[kk].start()
        if kk < n_blk - 1:
            forward(out0, True, 3 + kk)
            forward(out1, False, 3 + kk)
            forward(out1, True, 3 + kk)
        if kk == 0:
            shared_hidden(0, jn)
            shared_hidden(0, jf)

    near_sum(n_col - 1)

    outs = []
    for kk in range(n_col):
        ret_l[kk].wait_recv()
        ret_y[kk].wait_recv()
        cols = slice(kk * COL, (kk + 1) * COL)
        out_v[:, cols] = (x_all[0, my_rows, cols].astype(F32) + lacc[kk, c] + lrecv[kk] + yrecv[kk]).astype(BF16)
        outs.append(pltpu.make_async_copy(out_v.at[:, pl.ds(kk * COL, COL)], out.at[:, pl.ds(kk * COL, COL)], out_sem.at[kk]))
        outs[kk].start()

    for copy in [rt_p, rt_o, rt_f, x_p] + x_o + x_f + ret_p + ret_l + ret_y:
        copy.wait_send()
    for m in range(n_piece):
        for j, s in ((jn, s_near), (jf, s_far)):
            @pl.when(s != z)
            def _():
                send_x(j, m).wait_send()

            @pl.when(jnp.logical_and(z >= s, z < 3))
            def _():
                send_up(j, m).wait_send()

            @pl.when(jnp.logical_and(z <= s, z > 0))
            def _():
                send_down(j, m).wait_send()
    for copy in outs:
        copy.wait()


def solution(mesh):
    ep_size = mesh.shape["ep"]
    row_spec = P(("dp", "ep", "tp"), None)
    expert_spec = P("ep", None, None)

    def local_layer(tokens, expert_ids, gates, slots, sw1, sw3, sw2, ew1, ew3, ew2):
        n_tok, d_model = tokens.shape
        top_k = expert_ids.shape[1]
        n_exp, _, ff = ew1.shape
        cap = 8 * max(1, -(-2 * n_tok * top_k // (8 * n_exp * ep_size)))
        pair_rows = 2 * cap
        hid_w = sw1.shape[1] // 2
        n_blk, n_col = d_model // BLK, d_model // COL
        dma = pltpu.SemaphoreType.DMA
        vmem = pl.BlockSpec(memory_space=pltpu.VMEM)
        hbm = pl.BlockSpec(memory_space=pl.ANY)
        return pl.pallas_call(
            functools.partial(moe_kernel, cap),
            out_shape=jax.ShapeDtypeStruct((n_tok, d_model), BF16),
            in_specs=[vmem] * 3 + [hbm] * 7,
            out_specs=hbm,
            scratch_shapes=[
                pltpu.VMEM((2, 16, 2 * n_tok), F32),
                pltpu.VMEM((2, 2 * n_tok, d_model), BF16),
                pltpu.VMEM((2, n_exp * pair_rows, 2 * n_tok), BF16),
                pltpu.VMEM((n_exp, 2 * pair_rows, d_model), BF16),
                pltpu.VMEM((n_exp, 2 * pair_rows, ff), F32),
                pltpu.VMEM((n_exp, 2 * pair_rows, ff), F32),
                pltpu.VMEM((n_exp, 2 * pair_rows, ff), BF16),
                pltpu.VMEM((RING, GROUP, BLK, ff), BF16),
                pltpu.VMEM((2, 3, 2 * n_tok, n_exp * pair_rows), BF16),
                pltpu.VMEM((2, 3, n_exp * pair_rows, COL), BF16),
                pltpu.VMEM((d_model, 2 * hid_w), BF16),
                pltpu.VMEM((d_model, 2 * hid_w), BF16),
                pltpu.VMEM((2 * hid_w, d_model), BF16),
                pltpu.VMEM((2, 2 * n_tok, 2 * hid_w), BF16),
                pltpu.VMEM((n_col, 2, n_tok, COL), F32),
                pltpu.VMEM((n_col, 2, n_tok, COL), F32),
                pltpu.VMEM((n_col, n_tok, COL), F32),
                pltpu.VMEM((n_col, n_tok, COL), F32),
                pltpu.VMEM((n_col, n_tok, COL), F32),
                pltpu.VMEM((n_col, n_tok, COL), F32),
                pltpu.VMEM((n_tok, d_model), BF16),
                dma, dma((RING,)), dma((3,)), dma((4,)), dma((4,)),
                dma((n_blk,)), dma((n_blk,)), dma((n_blk,)), dma((n_blk,)),
                dma((2, 2 + n_blk)), dma((2, 2 + n_blk)), dma((2, 2 + n_blk)), dma((2, 2 + n_blk)), dma((2, 2 + n_blk)),
                dma((3, n_col)), dma((3, n_col)), dma((n_col,)),
            ],
            compiler_params=pltpu.CompilerParams(collective_id=0, has_side_effects=True, vmem_limit_bytes=67043328),
            name="moe_layer",
        )(expert_ids.T, gates.T, slots.T, tokens, sw1, sw3, sw2, ew1, ew3, ew2)

    return jax.shard_map(
        local_layer, mesh=mesh,
        in_specs=(row_spec, row_spec, row_spec, row_spec, P(None, "tp"), P(None, "tp"), P("tp", None), expert_spec, expert_spec, expert_spec),
        out_specs=row_spec, check_vma=False)
```

```python
import functools

import jax
import jax.numpy as jnp
from jax import lax
from jax.experimental import pallas as pl
from jax.experimental.pallas import tpu as pltpu
from jax.sharding import PartitionSpec as P

MESH = pl.DeviceIdType.MESH
BF16, F32 = jnp.bfloat16, jnp.float32
GROUP = 8
STEP = 8
RING = 8
BLK = 512
COL = 256


def dot(a, b):
    return jnp.dot(a, b, preferred_element_type=F32)


def glu(gate, up):
    return (gate * jax.nn.sigmoid(gate) * up).astype(BF16)


def moe_kernel(cap, ids_ref, gates_ref, slots_ref, tok, sw1, sw3, sw2, ew1, ew3, ew2, out,
               route, x_all, hot, xg, acc_g, acc_u, hid, ring, gt, rk, ws1, ws3, ws2, h_far, h_near, h_all,
               racc, lacc, precv, ysend, yrecv, lrecv,
               own_sem, ring_sem, loc_sem, rt_s, rt_r, xo_s, xo_r, xf_s, xf_r,
               zup_s, zdn_s, z_r, xs_s, xs_r, ret_s, ret_r, h_s, h_r):
    n_tok, d_model = tok.shape
    n_exp, _, ff = ew1.shape
    top_k = ids_ref.shape[0]
    pair_rows = 2 * cap
    half_d = d_model // 2
    hid_w = sw1.shape[1] // 2
    n_blk = d_model // BLK
    n_col = d_model // COL
    n_up = 2 * n_exp * n_blk
    n_load = n_up + n_exp * n_blk
    d, z, e = lax.axis_index("dp"), lax.axis_index("tp"), lax.axis_index("ep")
    c, y = lax.rem(e, 2), lax.div(e, 2)
    partner = {"ep": 2 * y + 1 - c}
    opp = {"ep": 2 * (1 - y) + c}
    x_peer = {"dp": 1 - d}
    up, down = {"tp": lax.rem(z + 1, 4)}, {"tp": lax.rem(z + 3, 4)}

    def span(i, n):
        return pl.ds(pl.multiple_of(i * n, n), n)

    my_rows = span(c, n_tok)

    def rdma(src, dst, send, recv, dev):
        return pltpu.make_async_remote_copy(src_ref=src, dst_ref=dst, send_sem=send, recv_sem=recv,
                                            device_id=dev, device_id_type=MESH)

    own = pltpu.make_async_copy(tok, x_all.at[0, my_rows, :], own_sem)
    own.start()

    r = 1 - c
    jn = lax.div(z, 2)
    jf = 1 - jn
    s_near = r + jn * (3 - 2 * r)
    s_far = r + jf * (3 - 2 * r)
    is_src = s_near == z
    n_piece = 2 + n_blk

    def own_copy(m):
        if m == 2:
            return pltpu.make_async_copy(sw2, ws2.at[span(jn, 2 * hid_w), :], loc_sem.at[m])
        return pltpu.make_async_copy((sw1, sw3)[m].at[:, span(y, hid_w)], (ws1, ws3)[m].at[jn], loc_sem.at[m])

    @pl.when(is_src)
    def _():
        for m in range(3):
            own_copy(m).start()

    def load(n):
        if n < n_up:
            kc, i, m = n // (2 * n_exp), n // 2 % n_exp, n % 2
            src = (ew1, ew3)[m].at[i, pl.ds(kc * BLK, BLK), :]
        else:
            src = ew2.at[(n - n_up) % n_exp, :, pl.ds((n - n_up) // n_exp * BLK, BLK)]
        group = n // GROUP % RING
        return pltpu.make_async_copy(src, ring.at[group, n % GROUP], ring_sem.at[group])

    def start_group(g):
        if g * GROUP < n_load:
            for n in range(g * GROUP, (g + 1) * GROUP):
                load(n).start()

    def wait_group(g):
        pltpu.make_async_copy(ring.at[g % RING], ring.at[g % RING], ring_sem.at[g % RING]).wait()

    def block(n):
        return ring.at[n // GROUP % RING, n % GROUP]

    ids, slots = ids_ref[...], slots_ref[...]
    code = jnp.where(slots >= 0, ids * pair_rows + c * cap + slots, -100000)
    route[0, 0:top_k, my_rows] = code.astype(F32)
    route[0, 8:8 + top_k, my_rows] = gates_ref[...]

    barrier = pltpu.get_barrier_semaphore()

    def greet(dev):
        pl.semaphore_signal(barrier, inc=1, device_id=dev, device_id_type=MESH)

    greet(partner)
    greet(opp)
    greet(x_peer)

    @pl.when(z < 3)
    def _():
        greet(up)

    @pl.when(z > 0)
    def _():
        greet(down)

    own.wait()
    start_group(0)
    pl.semaphore_wait(barrier, 4 + lax.rem(lax.div(z + 1, 2), 2))
    my_route = route.at[0, :, my_rows]
    far_route = route.at[1, :, my_rows]
    rt_p = rdma(my_route, my_route, rt_s.at[0], rt_r.at[0], partner)
    rt_o = rdma(my_route, far_route, rt_s.at[1], rt_r.at[1], opp)
    rt_f = rdma(far_route, far_route, rt_s.at[2], rt_r.at[2], partner)
    mine = x_all.at[0, my_rows, :]
    x_p = rdma(mine, mine, rt_s.at[3], rt_r.at[3], partner)
    x_o, x_f = [], []
    for q in range(n_blk):
        cols = pl.ds(q * BLK, BLK)
        there = x_all.at[1, my_rows, cols]
        x_o.append(rdma(x_all.at[0, my_rows, cols], there, xo_s.at[q], xo_r.at[q], opp))
        x_f.append(rdma(there, there, xf_s.at[q], xf_r.at[q], partner))
    x_o[0].start()
    rt_o.start()
    x_p.start()
    rt_p.start()

    def piece(j, m, half):
        if m >= 2:
            return ws2.at[span(2 * j + half, hid_w), pl.ds((m - 2) * BLK, BLK)]
        return (ws1, ws3)[m].at[j, span(half, half_d), :]

    def send_up(j, m):
        return rdma(piece(j, m, d), piece(j, m, d), zup_s.at[j, m], z_r.at[j, m], up)

    def send_down(j, m):
        return rdma(piece(j, m, d), piece(j, m, d), zdn_s.at[j, m], z_r.at[j, m], down)

    def send_x(j, m):
        return rdma(piece(j, m, d), piece(j, m, d), xs_s.at[j, m], xs_r.at[j, m], x_peer)

    inner = lax.rem(lax.div(z + 1, 2), 2) == 1
    outer = jnp.logical_not(inner)
    in0, in1 = jnp.logical_and(inner, r == 0), jnp.logical_and(inner, r == 1)
    out0, out1 = jnp.logical_and(outer, r == 0), jnp.logical_and(outer, r == 1)

    def from_source(cond, pieces, not_up=-1, not_down=-1):
        for m in pieces:
            @pl.when(jnp.logical_and(cond, jnp.logical_and(z < 3, z != not_up)))
            def _():
                send_up(jn, m).start()

            @pl.when(jnp.logical_and(cond, jnp.logical_and(z > 0, z != not_down)))
            def _():
                send_down(jn, m).start()

    def forward(cond, far, *pieces):
        j, s = (jf, s_far) if far else (jn, s_near)

        @pl.when(cond)
        def _():
            for m in pieces:
                send_up(j, m).wait_recv()

                @pl.when(jnp.logical_and(z > s, z < 3))
                def _():
                    send_up(j, m).start()

                @pl.when(jnp.logical_and(z < s, z > 0))
                def _():
                    send_down(j, m).start()

                send_x(j, m).start()

    w2_pieces = tuple(range(2, n_piece))

    @pl.when(is_src)
    def _():
        for m in range(3):
            own_copy(m).wait()

    from_source(is_src, (0, 1))
    from_source(out0, w2_pieces)
    for g in range(1, RING):
        start_group(g)

    base = (e * (n_exp * pair_rows)).astype(F32)

    def matches(p, first, n_rows, value):
        rows = lax.broadcasted_iota(jnp.int32, (n_rows, 2 * n_tok), 0).astype(F32) + (base + first)
        val = jnp.zeros((n_rows, 2 * n_tok), F32)
        for j in range(top_k):
            val = jnp.where(route[p, j:j + 1, :] == rows, value(j), val)
        return val

    def mark_rows(p):
        for g in range(n_exp // 4):
            n_rows = 4 * pair_rows
            hot[p, g * n_rows:(g + 1) * n_rows, :] = matches(p, g * n_rows, n_rows, lambda j: 1.0).astype(BF16)

    def place(p, kc):
        cols = slice(kc * BLK, (kc + 1) * BLK)
        for g in range(n_exp // 4):
            n_rows = 4 * pair_rows
            val = dot(hot[p, g * n_rows:(g + 1) * n_rows, :], x_all[p, :, cols]).astype(BF16)
            for q in range(4):
                xg[g * 4 + q, p * pair_rows:(p + 1) * pair_rows, cols] = val[q * pair_rows:(q + 1) * pair_rows]

    def gate_part(p, g):
        n_rows = 256
        val = matches(p, g * n_rows, n_rows, lambda j: route[p, 8 + j:9 + j, :]).T
        g1 = val.astype(BF16)
        rest = val - g1.astype(F32)
        g2 = rest.astype(BF16)
        g3 = (rest - g2.astype(F32)).astype(BF16)
        cols = slice(g * n_rows, (g + 1) * n_rows)
        gt[p, 0 * n_tok:2 * n_tok, cols] = g1
        gt[p, 2 * n_tok:4 * n_tok, cols] = g2
        gt[p, 4 * n_tok:6 * n_tok, cols] = g3

    def experts(kc, i0, extras):
        cols = slice(kc * BLK, (kc + 1) * BLK)
        group = (kc * 2 * n_exp + 2 * i0) // GROUP
        n_group = 2 * STEP // GROUP
        for g in range(group, group + n_group):
            wait_group(g)
        for i in range(i0, i0 + STEP):
            n = kc * 2 * n_exp + 2 * i
            rows = xg[i, :, cols]
            g = dot(rows, block(n)[...])
            u = dot(rows, block(n + 1)[...])
            if kc > 0:
                g, u = acc_g[i] + g, acc_u[i] + u
            if kc < n_blk - 1:
                acc_g[i] = g
                acc_u[i] = u
            else:
                hid[i] = glu(g, u)
        for extra in extras:
            extra()
        for g in range(group, group + n_group):
            start_group(g + RING)

    rt_p.wait_recv()
    x_p.wait_recv()
    mark_rows(0)
    place(0, 0)
    for g in range(n_exp * pair_rows // 256):
        gate_part(0, g)
    for q in range(1, n_blk):
        x_o[q].start()
    forward(in0, False, 0)
    forward(in1, True, 0)
    forward(out1, False, 0)
    rt_o.wait_recv()
    rt_f.start()
    x_o[0].wait_recv()
    x_f[0].start()
    for kc in range(1, n_blk):
        place(0, kc)
    forward(in0, False, 1)
    rt_f.wait_recv()
    mark_rows(1)
    n_gate = n_exp * pair_rows // 256

    def need_near(m):
        @pl.when(s_near != z)
        def _():
            send_x(jn, m).wait_recv()

    def need_far(m):
        send_x(jf, m).wait_recv()

    def shared_hidden(p, j):
        return glu(dot(x_all[p], ws1[j]), dot(x_all[p], ws3[j]))

    def h_out(j):
        return rdma(h_far.at[j], h_near.at[2 * j + y], h_s.at[j], h_r.at[j], opp)

    plan = {
        (0, 0): [(in1, True, 1), (out1, False, 1), (in0, True, 0)],
        (0, 8): [(out1, True, 0)],
        (1, 0): [(in0, True, 1), (in0, False) + w2_pieces],
        (2, 0): [(out1, True, 1), (in1, True) + w2_pieces],
        (2, 8): [(out0, True, 0)],
        0: [(out0, True, 1), (in0, True) + w2_pieces, (out1, False) + w2_pieces],
        2: [(out1, True) + w2_pieces],
        3: [(out0, True) + w2_pieces],
    }
    extras = {
        (1, 0): [functools.partial(gate_part, 1, g) for g in range(0, 2)],
        (1, 8): [functools.partial(gate_part, 1, g) for g in range(2, n_gate)],
    }
    for kc in range(n_blk):
        x_f[kc].wait_recv()
        place(1, kc)
        for i0 in range(0, n_exp, STEP):
            experts(kc, i0, extras.get((kc, i0), ()))
            for args in plan.get((kc, i0), ()):
                forward(*args)
            if (kc, i0) == (0, 0):
                from_source(in1, w2_pieces, not_up=2, not_down=1)
            if (kc, i0) == (1, 8):
                from_source(in1, w2_pieces, not_up=1, not_down=2)
            if (kc, i0) == (2, 0):
                need_near(0)
                need_near(1)
                h_far[jn] = shared_hidden(1, jn)
                h_out(jn).start()
            if i0 == 0 and kc + 1 < n_blk:
                x_o[kc + 1].wait_recv()
                x_f[kc + 1].start()

    def down_rows(kk):
        k, h = kk * COL // BLK, kk * COL % BLK
        if h == 0:
            for g in range(n_exp // GROUP):
                wait_group((n_up + k * n_exp) // GROUP + g)
        for i in range(n_exp):
            vals = dot(hid[i], block(n_up + k * n_exp + i)[:, h:h + COL]).astype(BF16)
            rows = pl.ds(i * pair_rows, pair_rows)
            rk[0, kk % 3, rows, :] = vals[0:pair_rows]
            rk[1, kk % 3, rows, :] = vals[pair_rows:]

    def combine(p, kk):
        sums = dot(gt[p], rk[p, kk % 3])
        return sums[0:2 * n_tok] + sums[2 * n_tok:4 * n_tok] + sums[4 * n_tok:]

    ret_p, ret_l, ret_y = [], [], []
    for kk in range(n_col):
        ret_p.append(rdma(racc.at[kk, 1 - c], precv.at[kk], ret_s.at[0, kk], ret_r.at[0, kk], partner))
        ret_l.append(rdma(lacc.at[kk, 1 - c], lrecv.at[kk], ret_s.at[1, kk], ret_r.at[1, kk], partner))
        ret_y.append(rdma(ysend.at[kk], yrecv.at[kk], ret_s.at[2, kk], ret_r.at[2, kk], opp))

    def far_sum(kk):
        total = combine(1, kk)
        racc[kk, 0] = total[0:n_tok]
        racc[kk, 1] = total[n_tok:]
        ret_p[kk].start()

    def near_sum(kk):
        total = combine(0, kk)
        lacc[kk, 0] = total[0:n_tok]
        lacc[kk, 1] = total[n_tok:]

    down_rows(0)
    for kk in range(n_col):
        far_sum(kk)
        if kk > 0:
            near_sum(kk - 1)
        if kk + 1 < n_col:
            down_rows(kk + 1)
        ret_p[kk].wait_recv()
        ysend[kk] = racc[kk, c] + precv[kk]
        ret_y[kk].start()
        for args in plan.get(kk, ()):
            forward(*args)
        if kk == 3:
            need_far(0)
            need_far(1)
            h_far[jf] = shared_hidden(1, jf)
            h_out(jf).start()
    near_sum(n_col - 1)
    for j in range(2):
        h_near[2 * j + y] = shared_hidden(0, j)
    for j in range(2):
        h_out(j).wait_recv()
    for q in range(4):
        h_all[:, q * hid_w:(q + 1) * hid_w] = h_near[q]
    for kk in range(n_col):
        if kk * COL % BLK == 0:
            need_near(2 + kk * COL // BLK)
            need_far(2 + kk * COL // BLK)
        part = dot(h_all[...], ws2[:, kk * COL:(kk + 1) * COL])
        lacc[kk, 0] = lacc[kk, 0] + part[0:n_tok]
        lacc[kk, 1] = lacc[kk, 1] + part[n_tok:]
        ret_l[kk].start()

    for kk in range(n_col):
        ret_l[kk].wait_recv()
        ret_y[kk].wait_recv()
        cols = slice(kk * COL, (kk + 1) * COL)
        out[:, cols] = (x_all[0, my_rows, cols].astype(F32) + lacc[kk, c] + lrecv[kk] + yrecv[kk]).astype(BF16)

    for copy in [rt_p, rt_o, rt_f, x_p] + x_o + x_f + ret_p + ret_l + ret_y + [h_out(0), h_out(1)]:
        copy.wait_send()
    for m in range(n_piece):
        for j, s in ((jn, s_near), (jf, s_far)):
            @pl.when(s != z)
            def _():
                send_x(j, m).wait_send()

            @pl.when(jnp.logical_and(z >= s, z < 3))
            def _():
                send_up(j, m).wait_send()

            @pl.when(jnp.logical_and(z <= s, z > 0))
            def _():
                send_down(j, m).wait_send()


def solution(mesh):
    ep_size = mesh.shape["ep"]
    row_spec = P(("dp", "ep", "tp"), None)
    expert_spec = P("ep", None, None)

    def local_layer(tokens, expert_ids, gates, slots, sw1, sw3, sw2, ew1, ew3, ew2):
        n_tok, d_model = tokens.shape
        top_k = expert_ids.shape[1]
        n_exp, _, ff = ew1.shape
        cap = 8 * max(1, -(-2 * n_tok * top_k // (8 * n_exp * ep_size)))
        pair_rows = 2 * cap
        hid_w = sw1.shape[1] // 2
        n_blk, n_col = d_model // BLK, d_model // COL
        dma = pltpu.SemaphoreType.DMA
        vmem = pl.BlockSpec(memory_space=pltpu.VMEM)
        hbm = pl.BlockSpec(memory_space=pl.ANY)
        return pl.pallas_call(
            functools.partial(moe_kernel, cap),
            out_shape=pltpu.VMEM((n_tok, d_model), BF16),
            in_specs=[vmem] * 3 + [hbm] * 7,
            out_specs=vmem,
            scratch_shapes=[
                pltpu.VMEM((2, 16, 2 * n_tok), F32),
                pltpu.VMEM((2, 2 * n_tok, d_model), BF16),
                pltpu.VMEM((2, n_exp * pair_rows, 2 * n_tok), BF16),
                pltpu.VMEM((n_exp, 2 * pair_rows, d_model), BF16),
                pltpu.VMEM((n_exp, 2 * pair_rows, ff), F32),
                pltpu.VMEM((n_exp, 2 * pair_rows, ff), F32),
                pltpu.VMEM((n_exp, 2 * pair_rows, ff), BF16),
                pltpu.VMEM((RING, GROUP, BLK, ff), BF16),
                pltpu.VMEM((2, 6 * n_tok, n_exp * pair_rows), BF16),
                pltpu.VMEM((2, 3, n_exp * pair_rows, COL), BF16),
                pltpu.VMEM((2, d_model, hid_w), BF16),
                pltpu.VMEM((2, d_model, hid_w), BF16),
                pltpu.VMEM((4 * hid_w, d_model), BF16),
                pltpu.VMEM((2, 2 * n_tok, hid_w), BF16),
                pltpu.VMEM((4, 2 * n_tok, hid_w), BF16),
                pltpu.VMEM((2 * n_tok, 4 * hid_w), BF16),
                pltpu.VMEM((n_col, 2, n_tok, COL), F32),
                pltpu.VMEM((n_col, 2, n_tok, COL), F32),
                pltpu.VMEM((n_col, n_tok, COL), F32),
                pltpu.VMEM((n_col, n_tok, COL), F32),
                pltpu.VMEM((n_col, n_tok, COL), F32),
                pltpu.VMEM((n_col, n_tok, COL), F32),
                dma, dma((RING,)), dma((3,)), dma((4,)), dma((4,)),
                dma((n_blk,)), dma((n_blk,)), dma((n_blk,)), dma((n_blk,)),
                dma((2, 2 + n_blk)), dma((2, 2 + n_blk)), dma((2, 2 + n_blk)), dma((2, 2 + n_blk)), dma((2, 2 + n_blk)),
                dma((3, n_col)), dma((3, n_col)), dma((2,)), dma((2,)),
            ],
            compiler_params=pltpu.CompilerParams(collective_id=0, has_side_effects=True, vmem_limit_bytes=66 * 1000 * 1000),
            name="moe_layer",
        )(expert_ids.T, gates.T, slots.T, tokens, sw1, sw3, sw2, ew1, ew3, ew2)

    return jax.shard_map(
        local_layer, mesh=mesh,
        in_specs=(row_spec, row_spec, row_spec, row_spec, P(None, "tp"), P(None, "tp"), P("tp", None), expert_spec, expert_spec, expert_spec),
        out_specs=row_spec, check_vma=False)
```

```python
import functools

import jax
import jax.numpy as jnp
from jax import lax
from jax.experimental import pallas as pl
from jax.experimental.pallas import tpu as pltpu
from jax.sharding import PartitionSpec as P

MESH = pl.DeviceIdType.MESH
BF16, F32 = jnp.bfloat16, jnp.float32
GROUP = 8
STEP = 8
RING = 8
BLK = 512
COL = 256


def dot(a, b):
    return jnp.dot(a, b, preferred_element_type=F32)


def glu(gate, up):
    return (gate * jax.nn.sigmoid(gate) * up).astype(BF16)


def moe_kernel(cap, ids_ref, gates_ref, slots_ref, tok, sw1, sw3, sw2, ew1, ew3, ew2, out,
               route, x_all, hot, xg, acc_g, acc_u, hid, ring, gt, rk, ws1, ws3, ws2, h_far, h_near, h_all,
               racc, lacc, precv, ysend, yrecv, lrecv,
               own_sem, ring_sem, loc_sem, rt_s, rt_r, xo_s, xo_r, xf_s, xf_r,
               zup_s, zdn_s, z_r, xs_s, xs_r, ret_s, ret_r, h_s, h_r):
    n_tok, d_model = tok.shape
    n_exp, _, ff = ew1.shape
    top_k = ids_ref.shape[0]
    pair_rows = 2 * cap
    half_d = d_model // 2
    hid_w = sw1.shape[1] // 2
    n_blk = d_model // BLK
    n_col = d_model // COL
    n_up = 2 * n_exp * n_blk
    n_load = n_up + n_exp * n_blk
    d, z, e = lax.axis_index("dp"), lax.axis_index("tp"), lax.axis_index("ep")
    c, y = lax.rem(e, 2), lax.div(e, 2)
    partner = {"ep": 2 * y + 1 - c}
    opp = {"ep": 2 * (1 - y) + c}
    x_peer = {"dp": 1 - d}
    up, down = {"tp": lax.rem(z + 1, 4)}, {"tp": lax.rem(z + 3, 4)}

    def span(i, n):
        return pl.ds(pl.multiple_of(i * n, n), n)

    my_rows = span(c, n_tok)

    def rdma(src, dst, send, recv, dev):
        return pltpu.make_async_remote_copy(src_ref=src, dst_ref=dst, send_sem=send, recv_sem=recv,
                                            device_id=dev, device_id_type=MESH)

    own = pltpu.make_async_copy(tok, x_all.at[0, my_rows, :], own_sem)
    own.start()

    r = 1 - c
    jn = lax.div(z, 2)
    jf = 1 - jn
    s_near = r + jn * (3 - 2 * r)
    s_far = r + jf * (3 - 2 * r)
    is_src = s_near == z
    n_piece = 2 + n_blk

    def own_copy(m):
        if m == 2:
            return pltpu.make_async_copy(sw2, ws2.at[span(jn, 2 * hid_w), :], loc_sem.at[m])
        return pltpu.make_async_copy((sw1, sw3)[m].at[:, span(y, hid_w)], (ws1, ws3)[m].at[jn], loc_sem.at[m])

    @pl.when(is_src)
    def _():
        for m in range(3):
            own_copy(m).start()

    def load(n):
        if n < n_up:
            kc, i, m = n // (2 * n_exp), n // 2 % n_exp, n % 2
            src = (ew1, ew3)[m].at[i, pl.ds(kc * BLK, BLK), :]
        else:
            src = ew2.at[(n - n_up) % n_exp, :, pl.ds((n - n_up) // n_exp * BLK, BLK)]
        group = n // GROUP % RING
        return pltpu.make_async_copy(src, ring.at[group, n % GROUP], ring_sem.at[group])

    def start_group(g):
        if g * GROUP < n_load:
            for n in range(g * GROUP, (g + 1) * GROUP):
                load(n).start()

    def wait_group(g):
        pltpu.make_async_copy(ring.at[g % RING], ring.at[g % RING], ring_sem.at[g % RING]).wait()

    def block(n):
        return ring.at[n // GROUP % RING, n % GROUP]

    ids, slots = ids_ref[...], slots_ref[...]
    code = jnp.where(slots >= 0, ids * pair_rows + c * cap + slots, -100000)
    route[0, 0:top_k, my_rows] = code.astype(F32)
    route[0, 8:8 + top_k, my_rows] = gates_ref[...]

    barrier = pltpu.get_barrier_semaphore()

    def greet(dev):
        pl.semaphore_signal(barrier, inc=1, device_id=dev, device_id_type=MESH)

    greet(partner)
    greet(opp)
    greet(x_peer)

    @pl.when(z < 3)
    def _():
        greet(up)

    @pl.when(z > 0)
    def _():
        greet(down)

    own.wait()
    start_group(0)
    pl.semaphore_wait(barrier, 4 + lax.rem(lax.div(z + 1, 2), 2))
    my_route = route.at[0, :, my_rows]
    far_route = route.at[1, :, my_rows]
    rt_p = rdma(my_route, my_route, rt_s.at[0], rt_r.at[0], partner)
    rt_o = rdma(my_route, far_route, rt_s.at[1], rt_r.at[1], opp)
    rt_f = rdma(far_route, far_route, rt_s.at[2], rt_r.at[2], partner)
    mine = x_all.at[0, my_rows, :]
    x_p = rdma(mine, mine, rt_s.at[3], rt_r.at[3], partner)
    x_o, x_f = [], []
    for q in range(n_blk):
        cols = pl.ds(q * BLK, BLK)
        there = x_all.at[1, my_rows, cols]
        x_o.append(rdma(x_all.at[0, my_rows, cols], there, xo_s, xo_r.at[q], opp))
        x_f.append(rdma(there, there, xf_s, xf_r.at[q], partner))
    rt_o.start()
    x_o[0].start()
    x_p.start()
    rt_p.start()

    def piece(j, m, half):
        if m >= 2:
            return ws2.at[span(2 * j + half, hid_w), pl.ds((m - 2) * BLK, BLK)]
        return (ws1, ws3)[m].at[j, span(half, half_d), :]

    def send_up(j, m):
        return rdma(piece(j, m, d), piece(j, m, d), zup_s.at[j], z_r.at[j, m], up)

    def send_down(j, m):
        return rdma(piece(j, m, d), piece(j, m, d), zdn_s.at[j], z_r.at[j, m], down)

    def send_x(j, m):
        return rdma(piece(j, m, d), piece(j, m, d), xs_s.at[j], xs_r.at[j, m], x_peer)

    inner = lax.rem(lax.div(z + 1, 2), 2) == 1
    outer = jnp.logical_not(inner)
    in0, in1 = jnp.logical_and(inner, r == 0), jnp.logical_and(inner, r == 1)
    out0, out1 = jnp.logical_and(outer, r == 0), jnp.logical_and(outer, r == 1)

    def from_source(cond, pieces, not_up=-1, not_down=-1):
        for m in pieces:
            @pl.when(jnp.logical_and(cond, jnp.logical_and(z < 3, z != not_up)))
            def _():
                send_up(jn, m).start()

            @pl.when(jnp.logical_and(cond, jnp.logical_and(z > 0, z != not_down)))
            def _():
                send_down(jn, m).start()

    def forward(cond, far, *pieces):
        j, s = (jf, s_far) if far else (jn, s_near)

        @pl.when(cond)
        def _():
            for m in pieces:
                send_up(j, m).wait_recv()

                @pl.when(jnp.logical_and(z > s, z < 3))
                def _():
                    send_up(j, m).start()

                @pl.when(jnp.logical_and(z < s, z > 0))
                def _():
                    send_down(j, m).start()

                send_x(j, m).start()

    w2_pieces = tuple(range(2, n_piece))

    @pl.when(is_src)
    def _():
        for m in range(3):
            own_copy(m).wait()

    from_source(is_src, (0, 1))
    from_source(out0, w2_pieces)
    for g in range(1, RING):
        start_group(g)

    base = (e * (n_exp * pair_rows)).astype(F32)

    def matches(p, first, n_rows, value):
        rows = lax.broadcasted_iota(jnp.int32, (n_rows, 2 * n_tok), 0).astype(F32) + (base + first)
        val = jnp.zeros((n_rows, 2 * n_tok), F32)
        for j in range(top_k):
            val = jnp.where(route[p, j:j + 1, :] == rows, value(j), val)
        return val

    def mark_rows(p):
        for g in range(n_exp // 4):
            n_rows = 4 * pair_rows
            hot[p, g * n_rows:(g + 1) * n_rows, :] = matches(p, g * n_rows, n_rows, lambda j: 1.0).astype(BF16)

    def place(p, kc):
        cols = slice(kc * BLK, (kc + 1) * BLK)
        for g in range(n_exp // 4):
            n_rows = 4 * pair_rows
            val = dot(hot[p, g * n_rows:(g + 1) * n_rows, :], x_all[p, :, cols]).astype(BF16)
            for q in range(4):
                xg[g * 4 + q, p * pair_rows:(p + 1) * pair_rows, cols] = val[q * pair_rows:(q + 1) * pair_rows]

    def gate_part(p, g):
        n_rows = 256
        val = matches(p, g * n_rows, n_rows, lambda j: route[p, 8 + j:9 + j, :]).T
        g1 = val.astype(BF16)
        rest = val - g1.astype(F32)
        g2 = rest.astype(BF16)
        g3 = (rest - g2.astype(F32)).astype(BF16)
        cols = slice(g * n_rows, (g + 1) * n_rows)
        gt[p, 0 * n_tok:2 * n_tok, cols] = g1
        gt[p, 2 * n_tok:4 * n_tok, cols] = g2
        gt[p, 4 * n_tok:6 * n_tok, cols] = g3

    def experts(kc, i0, extras):
        cols = slice(kc * BLK, (kc + 1) * BLK)
        group = (kc * 2 * n_exp + 2 * i0) // GROUP
        n_group = 2 * STEP // GROUP
        for g in range(group, group + n_group):
            wait_group(g)
        for i in range(i0, i0 + STEP):
            n = kc * 2 * n_exp + 2 * i
            rows = xg[i, :, cols]
            g = dot(rows, block(n)[...])
            u = dot(rows, block(n + 1)[...])
            if kc > 0:
                g, u = acc_g[i] + g, acc_u[i] + u
            if kc < n_blk - 1:
                acc_g[i] = g
                acc_u[i] = u
            else:
                hid[i] = glu(g, u)
        for extra in extras:
            extra()
        for g in range(group, group + n_group):
            start_group(g + RING)

    rt_p.wait_recv()
    x_p.wait_recv()
    mark_rows(0)
    place(0, 0)
    for g in range(n_exp * pair_rows // 256):
        gate_part(0, g)
    for q in range(1, n_blk):
        x_o[q].start()
    for kc in range(1, n_blk):
        place(0, kc)
    rt_o.wait_recv()
    rt_f.start()
    forward(in0, False, 0)
    rt_f.wait_recv()
    mark_rows(1)
    x_o[0].wait_recv()
    x_f[0].start()
    forward(in1, True, 0)
    forward(out1, False, 0)
    forward(in0, False, 1)
    n_gate = n_exp * pair_rows // 256

    def need_near(m):
        @pl.when(s_near != z)
        def _():
            send_x(jn, m).wait_recv()

    def need_far(m):
        send_x(jf, m).wait_recv()

    def shared_hidden(p, j):
        return glu(dot(x_all[p], ws1[j]), dot(x_all[p], ws3[j]))

    def h_out(j):
        return rdma(h_far.at[j], h_near.at[2 * j + y], h_s.at[j], h_r.at[j], opp)

    plan = {
        (0, 0): [(in1, True, 1), (out1, False, 1)],
        (0, 8): [(in0, True, 0)],
        (1, 0): [(in0, True, 1), (in0, False) + w2_pieces, (out1, True, 0)],
        (2, 0): [(out1, True, 1)],
        (2, 8): [(in1, True) + w2_pieces, (out0, True, 0)],
        0: [(out0, True, 1), (in0, True) + w2_pieces],
        1: [(out1, False) + w2_pieces],
        2: [(out1, True, 2)],
        3: [(out1, True, 3)],
        4: [(out1, True, 4), (out0, True) + w2_pieces],
    }
    extras = {
        (1, 0): [functools.partial(gate_part, 1, g) for g in range(0, 2)],
        (1, 8): [functools.partial(gate_part, 1, g) for g in range(2, n_gate)],
    }
    for kc in range(n_blk):
        x_f[kc].wait_recv()
        place(1, kc)
        for i0 in range(0, n_exp, STEP):
            experts(kc, i0, extras.get((kc, i0), ()))
            if i0 == 0 and kc + 1 < n_blk:
                x_o[kc + 1].wait_recv()
                x_f[kc + 1].start()
            for args in plan.get((kc, i0), ()):
                forward(*args)
            if (kc, i0) == (0, 0):
                from_source(in1, w2_pieces, not_up=2, not_down=1)
            if (kc, i0) == (1, 8):
                from_source(in1, w2_pieces, not_up=1, not_down=2)
            if (kc, i0) == (2, 0):
                need_near(0)
                need_near(1)
                h_far[jn] = shared_hidden(1, jn)
                h_out(jn).start()

    def down_rows(kk):
        k, h = kk * COL // BLK, kk * COL % BLK
        if h == 0:
            for g in range(n_exp // GROUP):
                wait_group((n_up + k * n_exp) // GROUP + g)
        for i in range(n_exp):
            vals = dot(hid[i], block(n_up + k * n_exp + i)[:, h:h + COL]).astype(BF16)
            rows = pl.ds(i * pair_rows, pair_rows)
            rk[0, kk % 3, rows, :] = vals[0:pair_rows]
            rk[1, kk % 3, rows, :] = vals[pair_rows:]

    def combine(p, kk, first, n):
        vals = rk[p, kk % 3]
        total = dot(gt[p, pl.ds(first, n)], vals)
        for m in range(1, 3):
            total += dot(gt[p, pl.ds(2 * m * n_tok + first, n)], vals)
        return total

    ret_p, ret_l, ret_y = [], [], []
    for kk in range(n_col):
        ret_p.append(rdma(racc.at[kk, 1 - c], precv.at[kk], ret_s.at[0], ret_r.at[0, kk], partner))
        ret_l.append(rdma(lacc.at[kk, 1 - c], lrecv.at[kk], ret_s.at[0], ret_r.at[1, kk], partner))
        ret_y.append(rdma(ysend.at[kk], yrecv.at[kk], ret_s.at[1], ret_r.at[2, kk], opp))

    def far_sum(kk):
        if kk == 0:
            for half in (1 - c, c):
                racc[kk, half] = combine(1, kk, pl.multiple_of(half * n_tok, n_tok), n_tok)
                if half is not c:
                    ret_p[kk].start()
        else:
            total = combine(1, kk, 0, 2 * n_tok)
            racc[kk, 0] = total[0:n_tok]
            racc[kk, 1] = total[n_tok:]
            ret_p[kk].start()

    def near_sum(kk):
        total = combine(0, kk, 0, 2 * n_tok)
        lacc[kk, 0] = total[0:n_tok]
        lacc[kk, 1] = total[n_tok:]

    down_rows(0)
    for kk in range(n_col):
        far_sum(kk)
        if kk > 0:
            near_sum(kk - 1)
        if kk + 1 < n_col:
            down_rows(kk + 1)
        ret_p[kk].wait_recv()
        ysend[kk] = racc[kk, c] + precv[kk]
        ret_y[kk].start()
        for args in plan.get(kk, ()):
            forward(*args)
        if kk == 3:
            need_far(0)
            need_far(1)
            h_far[jf] = shared_hidden(1, jf)
            h_out(jf).start()
    near_sum(n_col - 1)
    for j in range(2):
        h_near[2 * j + y] = shared_hidden(0, j)
    for j in range(2):
        h_out(j).wait_recv()
    for q in range(4):
        h_all[:, q * hid_w:(q + 1) * hid_w] = h_near[q]
    for kk in range(n_col):
        if kk * COL % BLK == 0:
            need_near(2 + kk * COL // BLK)
            need_far(2 + kk * COL // BLK)
        part = dot(h_all[...], ws2[:, kk * COL:(kk + 1) * COL])
        lacc[kk, 0] = lacc[kk, 0] + part[0:n_tok]
        lacc[kk, 1] = lacc[kk, 1] + part[n_tok:]
        ret_l[kk].start()

    for kk in range(n_col):
        ret_l[kk].wait_recv()
        ret_y[kk].wait_recv()
        cols = slice(kk * COL, (kk + 1) * COL)
        out[:, cols] = (x_all[0, my_rows, cols].astype(F32) + lacc[kk, c] + lrecv[kk] + yrecv[kk]).astype(BF16)

    def sent(ref, sem):
        pltpu.make_async_copy(ref, ref, sem).wait()

    for copy in [rt_p, rt_o, rt_f, x_p, h_out(0), h_out(1)]:
        copy.wait_send()
    sent(mine, xo_s)
    sent(mine, xf_s)
    sent(racc, ret_s.at[0])
    sent(ysend, ret_s.at[1])
    pieces = ws2.at[0:2 * hid_w, :]
    for j, s in ((jn, s_near), (jf, s_far)):
        @pl.when(s != z)
        def _():
            sent(pieces, xs_s.at[j])

        @pl.when(jnp.logical_and(z >= s, z < 3))
        def _():
            sent(pieces, zup_s.at[j])

        @pl.when(jnp.logical_and(z <= s, z > 0))
        def _():
            sent(pieces, zdn_s.at[j])


def solution(mesh):
    ep_size = mesh.shape["ep"]
    row_spec = P(("dp", "ep", "tp"), None)
    expert_spec = P("ep", None, None)

    def local_layer(tokens, expert_ids, gates, slots, sw1, sw3, sw2, ew1, ew3, ew2):
        n_tok, d_model = tokens.shape
        top_k = expert_ids.shape[1]
        n_exp, _, ff = ew1.shape
        cap = 8 * max(1, -(-2 * n_tok * top_k // (8 * n_exp * ep_size)))
        pair_rows = 2 * cap
        hid_w = sw1.shape[1] // 2
        n_blk, n_col = d_model // BLK, d_model // COL
        dma = pltpu.SemaphoreType.DMA
        vmem = pl.BlockSpec(memory_space=pltpu.VMEM)
        hbm = pl.BlockSpec(memory_space=pl.ANY)
        return pl.pallas_call(
            functools.partial(moe_kernel, cap),
            out_shape=pltpu.VMEM((n_tok, d_model), BF16),
            in_specs=[vmem] * 3 + [hbm] * 7,
            out_specs=vmem,
            scratch_shapes=[
                pltpu.VMEM((2, 16, 2 * n_tok), F32),
                pltpu.VMEM((2, 2 * n_tok, d_model), BF16),
                pltpu.VMEM((2, n_exp * pair_rows, 2 * n_tok), BF16),
                pltpu.VMEM((n_exp, 2 * pair_rows, d_model), BF16),
                pltpu.VMEM((n_exp, 2 * pair_rows, ff), F32),
                pltpu.VMEM((n_exp, 2 * pair_rows, ff), F32),
                pltpu.VMEM((n_exp, 2 * pair_rows, ff), BF16),
                pltpu.VMEM((RING, GROUP, BLK, ff), BF16),
                pltpu.VMEM((2, 6 * n_tok, n_exp * pair_rows), BF16),
                pltpu.VMEM((2, 3, n_exp * pair_rows, COL), BF16),
                pltpu.VMEM((2, d_model, hid_w), BF16),
                pltpu.VMEM((2, d_model, hid_w), BF16),
                pltpu.VMEM((4 * hid_w, d_model), BF16),
                pltpu.VMEM((2, 2 * n_tok, hid_w), BF16),
                pltpu.VMEM((4, 2 * n_tok, hid_w), BF16),
                pltpu.VMEM((2 * n_tok, 4 * hid_w), BF16),
                pltpu.VMEM((n_col, 2, n_tok, COL), F32),
                pltpu.VMEM((n_col, 2, n_tok, COL), F32),
                pltpu.VMEM((n_col, n_tok, COL), F32),
                pltpu.VMEM((n_col, n_tok, COL), F32),
                pltpu.VMEM((n_col, n_tok, COL), F32),
                pltpu.VMEM((n_col, n_tok, COL), F32),
                dma, dma((RING,)), dma((3,)), dma((4,)), dma((4,)),
                dma, dma((n_blk,)), dma, dma((n_blk,)),
                dma((2,)), dma((2,)), dma((2, 2 + n_blk)), dma((2,)), dma((2, 2 + n_blk)),
                dma((2,)), dma((3, n_col)), dma((2,)), dma((2,)),
            ],
            compiler_params=pltpu.CompilerParams(collective_id=0, has_side_effects=True, vmem_limit_bytes=66 * 1000 * 1000),
            name="moe_layer",
        )(expert_ids.T, gates.T, slots.T, tokens, sw1, sw3, sw2, ew1, ew3, ew2)

    return jax.shard_map(
        local_layer, mesh=mesh,
        in_specs=(row_spec, row_spec, row_spec, row_spec, P(None, "tp"), P(None, "tp"), P("tp", None), expert_spec, expert_spec, expert_spec),
        out_specs=row_spec, check_vma=False)
```

```python
import functools

import jax
import jax.numpy as jnp
from jax import lax
from jax.experimental import pallas as pl
from jax.experimental.pallas import tpu as pltpu
from jax.sharding import PartitionSpec as P

MESH = pl.DeviceIdType.MESH
BF16, F32 = jnp.bfloat16, jnp.float32
GROUP = 8
STEP = 8
RING = 8
BLK = 512
COL = 256


def dot(a, b):
    return jnp.dot(a, b, preferred_element_type=F32)


def glu(gate, up):
    return (gate * jax.nn.sigmoid(gate) * up).astype(BF16)


def moe_kernel(cap, ids_hbm, gates_hbm, slots_hbm, tok, sw1, sw3, sw2, ew1, ew3, ew2, out,
               ids_ref, gates_ref, slots_ref, route, x_all, hot, xg, acc_g, acc_u, hid, ring, gt, rk, ws1, ws3, ws2, h_far, h_near, h_all,
               racc, lacc, precv, ysend, yrecv, lrecv,
               own_sem, in_sem, ring_sem, down_sem, loc_sem, rt_s, rt_r, xo_s, xo_r, xf_s, xf_r,
               zup_s, zdn_s, z_r, xs_s, xs_r, ret_s, ret_r, h_s, h_r):
    n_tok, d_model = tok.shape
    n_exp, _, ff = ew1.shape
    top_k = ids_ref.shape[0]
    pair_rows = 2 * cap
    half_d = d_model // 2
    hid_w = sw1.shape[1] // 2
    n_blk = d_model // BLK
    n_col = d_model // COL
    n_up = 2 * n_exp * n_blk
    d, z, e = lax.axis_index("dp"), lax.axis_index("tp"), lax.axis_index("ep")
    c, y = lax.rem(e, 2), lax.div(e, 2)
    partner = {"ep": 2 * y + 1 - c}
    opp = {"ep": 2 * (1 - y) + c}
    x_peer = {"dp": 1 - d}
    up, down = {"tp": lax.rem(z + 1, 4)}, {"tp": lax.rem(z + 3, 4)}

    def span(i, n):
        return pl.ds(pl.multiple_of(i * n, n), n)

    my_rows = span(c, n_tok)

    def rdma(src, dst, send, recv, dev):
        return pltpu.make_async_remote_copy(src_ref=src, dst_ref=dst, send_sem=send, recv_sem=recv,
                                            device_id=dev, device_id_type=MESH)

    own = pltpu.make_async_copy(tok, x_all.at[0, my_rows, :], own_sem)
    own.start()
    small = [pltpu.make_async_copy(src, dst, in_sem.at[n]) for n, (src, dst) in enumerate(
        ((ids_hbm, ids_ref), (gates_hbm, gates_ref), (slots_hbm, slots_ref)))]
    for copy in small:
        copy.start()

    r = 1 - c
    jn = lax.div(z, 2)
    jf = 1 - jn
    s_near = r + jn * (3 - 2 * r)
    s_far = r + jf * (3 - 2 * r)
    is_src = s_near == z
    n_piece = 2 + n_blk

    def own_copy(m):
        if m == 2:
            return pltpu.make_async_copy(sw2, ws2.at[span(jn, 2 * hid_w), :], loc_sem.at[m])
        return pltpu.make_async_copy((sw1, sw3)[m].at[:, span(y, hid_w)], (ws1, ws3)[m].at[jn], loc_sem.at[m])

    @pl.when(is_src)
    def _():
        for m in range(3):
            own_copy(m).start()

    def start_group(g):
        for n in range(g * GROUP, (g + 1) * GROUP):
            kc, i, m = n // (2 * n_exp), n // 2 % n_exp, n % 2
            src = (ew1, ew3)[m].at[i, pl.ds(kc * BLK, BLK), :]
            pltpu.make_async_copy(src, ring.at[g % RING, n % GROUP], ring_sem.at[g % RING]).start()

    def wait_group(g):
        pltpu.make_async_copy(ring.at[g % RING], ring.at[g % RING], ring_sem.at[g % RING]).wait()

    def block(n):
        return ring.at[n // GROUP % RING, n % GROUP]

    def start_slab(k):
        for kk in range(k * BLK // COL, (k + 1) * BLK // COL):
            for i in range(n_exp):
                dst = block(n_up + k * n_exp + i).at[:, pl.ds(kk * COL % BLK, COL)]
                pltpu.make_async_copy(ew2.at[i, :, pl.ds(kk * COL, COL)], dst, down_sem.at[kk]).start()

    def wait_slab_part(kk):
        pltpu.make_async_copy(ring.at[0], ring.at[0], down_sem.at[kk]).wait()

    barrier = pltpu.get_barrier_semaphore()

    def greet(dev):
        pl.semaphore_signal(barrier, inc=1, device_id=dev, device_id_type=MESH)

    greet(partner)
    greet(opp)
    greet(x_peer)

    @pl.when(z < 3)
    def _():
        greet(up)

    @pl.when(z > 0)
    def _():
        greet(down)

    for copy in small:
        copy.wait()
    ids, slots = ids_ref[...], slots_ref[...]
    code = jnp.where(slots >= 0, ids * pair_rows + c * cap + slots, -100000)
    route[0, 0:top_k, my_rows] = code.astype(F32)
    route[0, 8:8 + top_k, my_rows] = gates_ref[...]
    own.wait()
    for g in range(3):
        start_group(g)
    pl.semaphore_wait(barrier, 4 + lax.rem(lax.div(z + 1, 2), 2))
    my_route = route.at[0, :, my_rows]
    far_route = route.at[1, :, my_rows]
    rt_p = rdma(my_route, my_route, rt_s.at[0], rt_r.at[0], partner)
    rt_o = rdma(my_route, far_route, rt_s.at[1], rt_r.at[1], opp)
    rt_f = rdma(far_route, far_route, rt_s.at[2], rt_r.at[2], partner)
    mine = x_all.at[0, my_rows, :]
    x_p = rdma(mine, mine, rt_s.at[3], rt_r.at[3], partner)
    x_o, x_f = [], []
    for q in range(n_blk):
        cols = pl.ds(q * BLK, BLK)
        there = x_all.at[1, my_rows, cols]
        x_o.append(rdma(x_all.at[0, my_rows, cols], there, xo_s, xo_r.at[q], opp))
        x_f.append(rdma(there, there, xf_s, xf_r.at[q], partner))
    rt_o.start()
    x_o[0].start()
    x_p.start()
    rt_p.start()

    def piece(j, m, half):
        if m >= 2:
            return ws2.at[span(2 * j + half, hid_w), pl.ds((m - 2) * BLK, BLK)]
        return (ws1, ws3)[m].at[j, span(half, half_d), :]

    def send_up(j, m):
        return rdma(piece(j, m, d), piece(j, m, d), zup_s.at[j], z_r.at[j, m], up)

    def send_down(j, m):
        return rdma(piece(j, m, d), piece(j, m, d), zdn_s.at[j], z_r.at[j, m], down)

    def send_x(j, m):
        return rdma(piece(j, m, d), piece(j, m, d), xs_s.at[j], xs_r.at[j, m], x_peer)

    inner = lax.rem(lax.div(z + 1, 2), 2) == 1
    outer = jnp.logical_not(inner)
    in0, in1 = jnp.logical_and(inner, r == 0), jnp.logical_and(inner, r == 1)
    out0, out1 = jnp.logical_and(outer, r == 0), jnp.logical_and(outer, r == 1)

    def from_source(cond, pieces, not_up=-1, not_down=-1):
        for m in pieces:
            @pl.when(jnp.logical_and(cond, jnp.logical_and(z < 3, z != not_up)))
            def _():
                send_up(jn, m).start()

            @pl.when(jnp.logical_and(cond, jnp.logical_and(z > 0, z != not_down)))
            def _():
                send_down(jn, m).start()

    def forward(cond, far, *pieces):
        j, s = (jf, s_far) if far else (jn, s_near)

        @pl.when(cond)
        def _():
            for m in pieces:
                send_up(j, m).wait_recv()

                @pl.when(jnp.logical_and(z > s, z < 3))
                def _():
                    send_up(j, m).start()

                @pl.when(jnp.logical_and(z < s, z > 0))
                def _():
                    send_down(j, m).start()

                send_x(j, m).start()

    w2_pieces = tuple(range(2, n_piece))

    @pl.when(is_src)
    def _():
        for m in range(3):
            own_copy(m).wait()

    from_source(is_src, (0, 1))
    from_source(out0, w2_pieces)
    for g in range(3, RING):
        start_group(g)

    base = (e * (n_exp * pair_rows)).astype(F32)

    def matches(p, first, n_rows, value):
        rows = lax.broadcasted_iota(jnp.int32, (n_rows, 2 * n_tok), 0).astype(F32) + (base + first)
        val = jnp.zeros((n_rows, 2 * n_tok), F32)
        for j in range(top_k):
            val = jnp.where(route[p, j:j + 1, :] == rows, value(j), val)
        return val

    def mark_rows(p):
        for g in range(n_exp // 4):
            n_rows = 4 * pair_rows
            hot[p, g * n_rows:(g + 1) * n_rows, :] = matches(p, g * n_rows, n_rows, lambda j: 1.0).astype(BF16)

    def place(p, kc):
        cols = slice(kc * BLK, (kc + 1) * BLK)
        for g in range(n_exp // 4):
            n_rows = 4 * pair_rows
            val = dot(hot[p, g * n_rows:(g + 1) * n_rows, :], x_all[p, :, cols]).astype(BF16)
            for q in range(4):
                xg[g * 4 + q, p * pair_rows:(p + 1) * pair_rows, cols] = val[q * pair_rows:(q + 1) * pair_rows]

    def gate_part(p, g):
        n_rows = 256
        val = matches(p, g * n_rows, n_rows, lambda j: route[p, 8 + j:9 + j, :]).T
        g1 = val.astype(BF16)
        rest = val - g1.astype(F32)
        g2 = rest.astype(BF16)
        g3 = (rest - g2.astype(F32)).astype(BF16)
        cols = slice(g * n_rows, (g + 1) * n_rows)
        gt[p, 0 * n_tok:2 * n_tok, cols] = g1
        gt[p, 2 * n_tok:4 * n_tok, cols] = g2
        gt[p, 4 * n_tok:6 * n_tok, cols] = g3

    def experts(kc, i0, extras):
        cols = slice(kc * BLK, (kc + 1) * BLK)
        group = (kc * 2 * n_exp + 2 * i0) // GROUP
        n_group = 2 * STEP // GROUP
        for g in range(group, group + n_group):
            wait_group(g)
        for i in range(i0, i0 + STEP):
            n = kc * 2 * n_exp + 2 * i
            rows = xg[i, :, cols]
            g = dot(rows, block(n)[...])
            u = dot(rows, block(n + 1)[...])
            if kc > 0:
                g, u = acc_g[i] + g, acc_u[i] + u
            if kc < n_blk - 1:
                acc_g[i] = g
                acc_u[i] = u
            else:
                hid[i] = glu(g, u)
        for extra in extras:
            extra()
        ahead = (group + RING) * GROUP
        if ahead < n_up:
            for g in range(group, group + n_group):
                start_group(g + RING)
        elif ahead - n_up < n_blk * n_exp:
            start_slab((ahead - n_up) // n_exp)

    rt_p.wait_recv()
    x_p.wait_recv()
    mark_rows(0)
    place(0, 0)
    for g in range(n_exp * pair_rows // 256):
        gate_part(0, g)
    for q in range(1, n_blk):
        x_o[q].start()
    for kc in range(1, n_blk):
        place(0, kc)
    rt_o.wait_recv()
    rt_f.start()
    forward(in0, False, 0)
    rt_f.wait_recv()
    mark_rows(1)
    x_o[0].wait_recv()
    x_f[0].start()
    forward(in1, True, 0)
    forward(out1, False, 0)
    forward(in0, False, 1)
    n_gate = n_exp * pair_rows // 256

    def need_near(m):
        @pl.when(s_near != z)
        def _():
            send_x(jn, m).wait_recv()

    def need_far(m):
        send_x(jf, m).wait_recv()

    def shared_hidden(p, j):
        return glu(dot(x_all[p], ws1[j]), dot(x_all[p], ws3[j]))

    def h_out(j):
        return rdma(h_far.at[j], h_near.at[2 * j + y], h_s.at[j], h_r.at[j], opp)

    plan = {
        (0, 0): [(in1, True, 1), (out1, False, 1)],
        (0, 8): [(in0, True, 0)],
        (1, 0): [(in0, True, 1), (in0, False) + w2_pieces, (out1, True, 0)],
        (2, 0): [(out1, True, 1)],
        (2, 8): [(in1, True) + w2_pieces, (out0, True, 0)],
        0: [(out0, True, 1), (in0, True) + w2_pieces],
        1: [(out1, False) + w2_pieces],
        2: [(out1, True, 2)],
        3: [(out1, True, 3)],
        4: [(out1, True, 4), (out0, True) + w2_pieces],
    }
    extras = {
        (1, 0): [functools.partial(gate_part, 1, g) for g in range(0, 2)],
        (1, 8): [functools.partial(gate_part, 1, g) for g in range(2, n_gate)],
    }
    for kc in range(n_blk):
        x_f[kc].wait_recv()
        place(1, kc)
        for i0 in range(0, n_exp, STEP):
            experts(kc, i0, extras.get((kc, i0), ()))
            if i0 == 0 and kc + 1 < n_blk:
                x_o[kc + 1].wait_recv()
                x_f[kc + 1].start()
            for args in plan.get((kc, i0), ()):
                forward(*args)
            if (kc, i0) == (0, 0):
                from_source(in1, w2_pieces, not_up=2, not_down=1)
            if (kc, i0) == (1, 8):
                from_source(in1, w2_pieces, not_up=1, not_down=2)
            if (kc, i0) == (2, 0):
                need_near(0)
                need_near(1)
                h_far[jn] = shared_hidden(1, jn)
                h_out(jn).start()

    def down_rows(kk):
        k, h = kk * COL // BLK, kk * COL % BLK
        wait_slab_part(kk)
        for i in range(n_exp):
            vals = dot(hid[i], block(n_up + k * n_exp + i)[:, h:h + COL]).astype(BF16)
            rows = pl.ds(i * pair_rows, pair_rows)
            rk[0, kk % 3, rows, :] = vals[0:pair_rows]
            rk[1, kk % 3, rows, :] = vals[pair_rows:]

    def combine(p, kk, first, n):
        vals = rk[p, kk % 3]
        total = dot(gt[p, pl.ds(first, n)], vals)
        for m in range(1, 3):
            total += dot(gt[p, pl.ds(2 * m * n_tok + first, n)], vals)
        return total

    ret_p, ret_l, ret_y = [], [], []
    for kk in range(n_col):
        ret_p.append(rdma(racc.at[kk, 1 - c], precv.at[kk], ret_s.at[0], ret_r.at[0, kk], partner))
        ret_l.append(rdma(lacc.at[kk, 1 - c], lrecv.at[kk], ret_s.at[0], ret_r.at[1, kk], partner))
        ret_y.append(rdma(ysend.at[kk], yrecv.at[kk], ret_s.at[1], ret_r.at[2, kk], opp))

    def far_sum(kk):
        if kk == 0:
            for half in (1 - c, c):
                racc[kk, half] = combine(1, kk, pl.multiple_of(half * n_tok, n_tok), n_tok)
                if half is not c:
                    ret_p[kk].start()
        else:
            total = combine(1, kk, 0, 2 * n_tok)
            racc[kk, 0] = total[0:n_tok]
            racc[kk, 1] = total[n_tok:]
            ret_p[kk].start()

    def near_sum(kk):
        total = combine(0, kk, 0, 2 * n_tok)
        lacc[kk, 0] = total[0:n_tok]
        lacc[kk, 1] = total[n_tok:]

    down_rows(0)
    for kk in range(n_col):
        far_sum(kk)
        if kk > 0:
            near_sum(kk - 1)
        if kk + 1 < n_col:
            down_rows(kk + 1)
        ret_p[kk].wait_recv()
        ysend[kk] = racc[kk, c] + precv[kk]
        ret_y[kk].start()
        for args in plan.get(kk, ()):
            forward(*args)
        if kk == 3:
            need_far(0)
            need_far(1)
            h_far[jf] = shared_hidden(1, jf)
            h_out(jf).start()
    near_sum(n_col - 1)
    for j in range(2):
        h_near[2 * j + y] = shared_hidden(0, j)
    for j in range(2):
        h_out(j).wait_recv()
    for q in range(4):
        h_all[:, q * hid_w:(q + 1) * hid_w] = h_near[q]
    for kk in range(n_col):
        if kk * COL % BLK == 0:
            need_near(2 + kk * COL // BLK)
            need_far(2 + kk * COL // BLK)
        part = dot(h_all[...], ws2[:, kk * COL:(kk + 1) * COL])
        lacc[kk, 0] = lacc[kk, 0] + part[0:n_tok]
        lacc[kk, 1] = lacc[kk, 1] + part[n_tok:]
        ret_l[kk].start()

    for kk in range(n_col):
        ret_l[kk].wait_recv()
        ret_y[kk].wait_recv()
        cols = slice(kk * COL, (kk + 1) * COL)
        out[:, cols] = (x_all[0, my_rows, cols].astype(F32) + lacc[kk, c] + lrecv[kk] + yrecv[kk]).astype(BF16)

    def sent(ref, sem):
        pltpu.make_async_copy(ref, ref, sem).wait()

    for copy in [rt_p, rt_o, rt_f, x_p, h_out(0), h_out(1)]:
        copy.wait_send()
    sent(mine, xo_s)
    sent(mine, xf_s)
    sent(racc, ret_s.at[0])
    sent(ysend, ret_s.at[1])
    pieces = ws2.at[0:2 * hid_w, :]
    for j, s in ((jn, s_near), (jf, s_far)):
        @pl.when(s != z)
        def _():
            sent(pieces, xs_s.at[j])

        @pl.when(jnp.logical_and(z >= s, z < 3))
        def _():
            sent(pieces, zup_s.at[j])

        @pl.when(jnp.logical_and(z <= s, z > 0))
        def _():
            sent(pieces, zdn_s.at[j])


def solution(mesh):
    ep_size = mesh.shape["ep"]
    row_spec = P(("dp", "ep", "tp"), None)
    expert_spec = P("ep", None, None)

    def local_layer(tokens, expert_ids, gates, slots, sw1, sw3, sw2, ew1, ew3, ew2):
        n_tok, d_model = tokens.shape
        top_k = expert_ids.shape[1]
        n_exp, _, ff = ew1.shape
        cap = 8 * max(1, -(-2 * n_tok * top_k // (8 * n_exp * ep_size)))
        pair_rows = 2 * cap
        hid_w = sw1.shape[1] // 2
        n_blk, n_col = d_model // BLK, d_model // COL
        dma = pltpu.SemaphoreType.DMA
        vmem = pl.BlockSpec(memory_space=pltpu.VMEM)
        hbm = pl.BlockSpec(memory_space=pl.ANY)
        return pl.pallas_call(
            functools.partial(moe_kernel, cap),
            out_shape=pltpu.VMEM((n_tok, d_model), BF16),
            in_specs=[hbm] * 10,
            out_specs=vmem,
            scratch_shapes=[
                pltpu.VMEM((top_k, n_tok), jnp.int32), pltpu.VMEM((top_k, n_tok), F32), pltpu.VMEM((top_k, n_tok), jnp.int32),
                pltpu.VMEM((2, 16, 2 * n_tok), F32),
                pltpu.VMEM((2, 2 * n_tok, d_model), BF16),
                pltpu.VMEM((2, n_exp * pair_rows, 2 * n_tok), BF16),
                pltpu.VMEM((n_exp, 2 * pair_rows, d_model), BF16),
                pltpu.VMEM((n_exp, 2 * pair_rows, ff), F32),
                pltpu.VMEM((n_exp, 2 * pair_rows, ff), F32),
                pltpu.VMEM((n_exp, 2 * pair_rows, ff), BF16),
                pltpu.VMEM((RING, GROUP, BLK, ff), BF16),
                pltpu.VMEM((2, 6 * n_tok, n_exp * pair_rows), BF16),
                pltpu.VMEM((2, 3, n_exp * pair_rows, COL), BF16),
                pltpu.VMEM((2, d_model, hid_w), BF16),
                pltpu.VMEM((2, d_model, hid_w), BF16),
                pltpu.VMEM((4 * hid_w, d_model), BF16),
                pltpu.VMEM((2, 2 * n_tok, hid_w), BF16),
                pltpu.VMEM((4, 2 * n_tok, hid_w), BF16),
                pltpu.VMEM((2 * n_tok, 4 * hid_w), BF16),
                pltpu.VMEM((n_col, 2, n_tok, COL), F32),
                pltpu.VMEM((n_col, 2, n_tok, COL), F32),
                pltpu.VMEM((n_col, n_tok, COL), F32),
                pltpu.VMEM((n_col, n_tok, COL), F32),
                pltpu.VMEM((n_col, n_tok, COL), F32),
                pltpu.VMEM((n_col, n_tok, COL), F32),
                dma, dma((3,)), dma((RING,)), dma((n_col,)), dma((3,)), dma((4,)), dma((4,)),
                dma, dma((n_blk,)), dma, dma((n_blk,)),
                dma((2,)), dma((2,)), dma((2, 2 + n_blk)), dma((2,)), dma((2, 2 + n_blk)),
                dma((2,)), dma((3, n_col)), dma((2,)), dma((2,)),
            ],
            compiler_params=pltpu.CompilerParams(collective_id=0, has_side_effects=True, vmem_limit_bytes=66 * 1000 * 1000),
            name="moe_layer",
        )(expert_ids.T, gates.T, slots.T, tokens, sw1, sw3, sw2, ew1, ew3, ew2)

    return jax.shard_map(
        local_layer, mesh=mesh,
        in_specs=(row_spec, row_spec, row_spec, row_spec, P(None, "tp"), P(None, "tp"), P("tp", None), expert_spec, expert_spec, expert_spec),
        out_specs=row_spec, check_vma=False)
```

```python
import functools

import jax
import jax.numpy as jnp
from jax import lax
from jax.experimental import pallas as pl
from jax.experimental.pallas import tpu as pltpu
from jax.sharding import PartitionSpec as P

MESH = pl.DeviceIdType.MESH
BF16, F32 = jnp.bfloat16, jnp.float32
GROUP = 8
STEP = 8
RING = 8
BLK = 512
COL = 256


def dot(a, b):
    return jnp.dot(a, b, preferred_element_type=F32)


def glu(gate, up):
    return (gate * jax.nn.sigmoid(gate) * up).astype(BF16)


def moe_kernel(cap, ids_hbm, gates_hbm, slots_hbm, tok, sw1, sw3, sw2, ew1, ew3, ew2, out,
               ids_ref, gates_ref, slots_ref, route, x_all, hot, xg, acc_g, acc_u, hid, ring, gt, rk, ws1, ws3, ws2, h_far, h_near, h_all,
               racc, lacc, precv, ysend, yrecv, lrecv,
               own_sem, in_sem, ring_sem, down_sem, loc_sem, rt_s, rt_r, xo_s, xo_r, xf_s, xf_r,
               zup_s, zdn_s, z_r, xs_s, xs_r, ret_s, ret_r, h_s, h_r):
    n_tok, d_model = tok.shape
    n_exp, _, ff = ew1.shape
    top_k = ids_ref.shape[0]
    pair_rows = 2 * cap
    half_d = d_model // 2
    hid_w = sw1.shape[1] // 2
    n_blk = d_model // BLK
    n_col = d_model // COL
    n_up = 2 * n_exp * n_blk
    d, z, e = lax.axis_index("dp"), lax.axis_index("tp"), lax.axis_index("ep")
    c, y = lax.rem(e, 2), lax.div(e, 2)
    partner = {"ep": 2 * y + 1 - c}
    opp = {"ep": 2 * (1 - y) + c}
    x_peer = {"dp": 1 - d}
    up, down = {"tp": lax.rem(z + 1, 4)}, {"tp": lax.rem(z + 3, 4)}

    def span(i, n):
        return pl.ds(pl.multiple_of(i * n, n), n)

    my_rows = span(c, n_tok)

    def rdma(src, dst, send, recv, dev):
        return pltpu.make_async_remote_copy(src_ref=src, dst_ref=dst, send_sem=send, recv_sem=recv,
                                            device_id=dev, device_id_type=MESH)

    own = pltpu.make_async_copy(tok, x_all.at[0, my_rows, :], own_sem)
    own.start()
    small = [pltpu.make_async_copy(src, dst, in_sem.at[n]) for n, (src, dst) in enumerate(
        ((ids_hbm, ids_ref), (gates_hbm, gates_ref), (slots_hbm, slots_ref)))]
    for copy in small:
        copy.start()

    r = 1 - c
    jn = lax.div(z, 2)
    jf = 1 - jn
    s_near = r + jn * (3 - 2 * r)
    s_far = r + jf * (3 - 2 * r)
    is_src = s_near == z
    n_piece = 2 + n_blk

    def own_copy(m):
        if m == 2:
            return pltpu.make_async_copy(sw2, ws2.at[span(jn, 2 * hid_w), :], loc_sem.at[m])
        return pltpu.make_async_copy((sw1, sw3)[m].at[:, span(y, hid_w)], (ws1, ws3)[m].at[jn], loc_sem.at[m])

    @pl.when(is_src)
    def _():
        for m in range(3):
            own_copy(m).start()

    def start_group(g):
        for n in range(g * GROUP, (g + 1) * GROUP):
            kc, i, m = n // (2 * n_exp), n // 2 % n_exp, n % 2
            src = (ew1, ew3)[m].at[i, pl.ds(kc * BLK, BLK), :]
            pltpu.make_async_copy(src, ring.at[g % RING, n % GROUP], ring_sem.at[g % RING]).start()

    def wait_group(g):
        pltpu.make_async_copy(ring.at[g % RING], ring.at[g % RING], ring_sem.at[g % RING]).wait()

    def block(n):
        return ring.at[n // GROUP % RING, n % GROUP]

    def start_slab(k):
        for kk in range(k * BLK // COL, (k + 1) * BLK // COL):
            for i in range(n_exp):
                dst = block(n_up + k * n_exp + i).at[:, pl.ds(kk * COL % BLK, COL)]
                pltpu.make_async_copy(ew2.at[i, :, pl.ds(kk * COL, COL)], dst, down_sem.at[kk]).start()

    def wait_slab_part(kk):
        pltpu.make_async_copy(ring.at[0], ring.at[0], down_sem.at[kk]).wait()

    barrier = pltpu.get_barrier_semaphore()

    def greet(dev):
        pl.semaphore_signal(barrier, inc=1, device_id=dev, device_id_type=MESH)

    greet(partner)
    greet(opp)
    greet(x_peer)

    @pl.when(z < 3)
    def _():
        greet(up)

    @pl.when(z > 0)
    def _():
        greet(down)

    start_group(0)
    for copy in small:
        copy.wait()
    ids, slots = ids_ref[...], slots_ref[...]
    code = jnp.where(slots >= 0, ids * pair_rows + c * cap + slots, -100000)
    route[0, 0:top_k, my_rows] = code.astype(F32)
    route[0, 8:8 + top_k, my_rows] = gates_ref[...]
    own.wait()
    for g in range(1, 3):
        start_group(g)
    pl.semaphore_wait(barrier, 4 + lax.rem(lax.div(z + 1, 2), 2))
    my_route = route.at[0, :, my_rows]
    far_route = route.at[1, :, my_rows]
    rt_p = rdma(my_route, my_route, rt_s.at[0], rt_r.at[0], partner)
    rt_o = rdma(my_route, far_route, rt_s.at[1], rt_r.at[1], opp)
    rt_f = rdma(far_route, far_route, rt_s.at[2], rt_r.at[2], partner)
    mine = x_all.at[0, my_rows, :]
    x_p = rdma(mine, mine, rt_s.at[3], rt_r.at[3], partner)
    x_o, x_f = [], []
    for q in range(n_blk):
        cols = pl.ds(q * BLK, BLK)
        there = x_all.at[1, my_rows, cols]
        x_o.append(rdma(x_all.at[0, my_rows, cols], there, xo_s, xo_r.at[q], opp))
        x_f.append(rdma(there, there, xf_s, xf_r.at[q], partner))
    rt_o.start()
    x_o[0].start()
    x_p.start()
    rt_p.start()

    def piece(j, m, half):
        if m >= 2:
            return ws2.at[span(2 * j + half, hid_w), pl.ds((m - 2) * BLK, BLK)]
        return (ws1, ws3)[m].at[j, span(half, half_d), :]

    def send_up(j, m):
        return rdma(piece(j, m, d), piece(j, m, d), zup_s.at[j], z_r.at[j, m], up)

    def send_down(j, m):
        return rdma(piece(j, m, d), piece(j, m, d), zdn_s.at[j], z_r.at[j, m], down)

    def send_x(j, m):
        return rdma(piece(j, m, d), piece(j, m, d), xs_s.at[j], xs_r.at[j, m], x_peer)

    inner = lax.rem(lax.div(z + 1, 2), 2) == 1
    outer = jnp.logical_not(inner)
    in0, in1 = jnp.logical_and(inner, r == 0), jnp.logical_and(inner, r == 1)
    out0, out1 = jnp.logical_and(outer, r == 0), jnp.logical_and(outer, r == 1)

    def from_source(cond, pieces, not_up=-1, not_down=-1):
        for m in pieces:
            @pl.when(jnp.logical_and(cond, jnp.logical_and(z < 3, z != not_up)))
            def _():
                send_up(jn, m).start()

            @pl.when(jnp.logical_and(cond, jnp.logical_and(z > 0, z != not_down)))
            def _():
                send_down(jn, m).start()

    def forward(cond, far, *pieces):
        j, s = (jf, s_far) if far else (jn, s_near)

        @pl.when(cond)
        def _():
            for m in pieces:
                send_up(j, m).wait_recv()

                @pl.when(jnp.logical_and(z > s, z < 3))
                def _():
                    send_up(j, m).start()

                @pl.when(jnp.logical_and(z < s, z > 0))
                def _():
                    send_down(j, m).start()

                send_x(j, m).start()

    w2_pieces = tuple(range(2, n_piece))

    @pl.when(is_src)
    def _():
        for m in range(3):
            own_copy(m).wait()

    from_source(is_src, (0, 1))
    from_source(out0, w2_pieces)
    for g in range(3, RING):
        start_group(g)

    base = (e * (n_exp * pair_rows)).astype(F32)

    def matches(p, first, n_rows, value):
        rows = lax.broadcasted_iota(jnp.int32, (n_rows, 2 * n_tok), 0).astype(F32) + (base + first)
        val = jnp.zeros((n_rows, 2 * n_tok), F32)
        for j in range(top_k):
            val = jnp.where(route[p, j:j + 1, :] == rows, value(j), val)
        return val

    def mark_rows(p):
        for g in range(n_exp // 4):
            n_rows = 4 * pair_rows
            hot[p, g * n_rows:(g + 1) * n_rows, :] = matches(p, g * n_rows, n_rows, lambda j: 1.0).astype(BF16)

    def place(p, kc):
        cols = slice(kc * BLK, (kc + 1) * BLK)
        for g in range(n_exp // 4):
            n_rows = 4 * pair_rows
            val = dot(hot[p, g * n_rows:(g + 1) * n_rows, :], x_all[p, :, cols]).astype(BF16)
            for q in range(4):
                xg[g * 4 + q, p * pair_rows:(p + 1) * pair_rows, cols] = val[q * pair_rows:(q + 1) * pair_rows]

    def gate_part(p, g):
        n_rows = 256
        val = matches(p, g * n_rows, n_rows, lambda j: route[p, 8 + j:9 + j, :]).T
        g1 = val.astype(BF16)
        rest = val - g1.astype(F32)
        g2 = rest.astype(BF16)
        g3 = (rest - g2.astype(F32)).astype(BF16)
        cols = slice(g * n_rows, (g + 1) * n_rows)
        gt[p, 0 * n_tok:2 * n_tok, cols] = g1
        gt[p, 2 * n_tok:4 * n_tok, cols] = g2
        gt[p, 4 * n_tok:6 * n_tok, cols] = g3

    def experts(kc, i0, extras):
        cols = slice(kc * BLK, (kc + 1) * BLK)
        group = (kc * 2 * n_exp + 2 * i0) // GROUP
        n_group = 2 * STEP // GROUP
        for g in range(group, group + n_group):
            wait_group(g)
        for i in range(i0, i0 + STEP):
            n = kc * 2 * n_exp + 2 * i
            rows = xg[i, :, cols]
            g = dot(rows, block(n)[...])
            u = dot(rows, block(n + 1)[...])
            if kc > 0:
                g, u = acc_g[i] + g, acc_u[i] + u
            if kc < n_blk - 1:
                acc_g[i] = g
                acc_u[i] = u
            else:
                hid[i] = glu(g, u)
        for extra in extras:
            extra()
        ahead = (group + RING) * GROUP
        if ahead < n_up:
            for g in range(group, group + n_group):
                start_group(g + RING)
        elif ahead - n_up < n_blk * n_exp:
            start_slab((ahead - n_up) // n_exp)

    rt_p.wait_recv()
    x_p.wait_recv()
    mark_rows(0)
    place(0, 0)
    for g in range(n_exp * pair_rows // 256):
        gate_part(0, g)
    for q in range(1, n_blk):
        x_o[q].start()
    for kc in range(1, n_blk):
        place(0, kc)
    rt_o.wait_recv()
    rt_f.start()
    forward(in0, False, 0)
    rt_f.wait_recv()
    mark_rows(1)
    x_o[0].wait_recv()
    x_f[0].start()
    forward(in1, True, 0)
    forward(out1, False, 0)
    forward(in0, False, 1)
    n_gate = n_exp * pair_rows // 256

    def need_near(m):
        @pl.when(s_near != z)
        def _():
            send_x(jn, m).wait_recv()

    def need_far(m):
        send_x(jf, m).wait_recv()

    def shared_hidden(p, j):
        return glu(dot(x_all[p], ws1[j]), dot(x_all[p], ws3[j]))

    def h_out(j):
        return rdma(h_far.at[j], h_near.at[2 * j + y], h_s.at[j], h_r.at[j], opp)

    plan = {
        (0, 0): [(in1, True, 1), (out1, False, 1)],
        (0, 8): [(in0, True, 0)],
        (1, 0): [(in0, True, 1), (in0, False) + w2_pieces, (out1, True, 0)],
        (2, 0): [(out1, True, 1)],
        (2, 8): [(in1, True) + w2_pieces, (out0, True, 0)],
        0: [(out0, True, 1), (in0, True) + w2_pieces],
        1: [(out1, False) + w2_pieces],
        2: [(out1, True, 2)],
        3: [(out1, True, 3)],
        4: [(out1, True, 4), (out0, True) + w2_pieces],
    }
    def near_hidden():
        h_far[jn] = shared_hidden(1, jn)

    extras = {
        (1, 0): [functools.partial(gate_part, 1, g) for g in range(0, 2)],
        (1, 8): [functools.partial(gate_part, 1, g) for g in range(2, n_gate)],
        (2, 8): [near_hidden],
    }
    for kc in range(n_blk):
        x_f[kc].wait_recv()
        place(1, kc)
        for i0 in range(0, n_exp, STEP):
            if (kc, i0) == (2, 8):
                need_near(0)
                need_near(1)
            experts(kc, i0, extras.get((kc, i0), ()))
            if i0 == 0 and kc + 1 < n_blk:
                x_o[kc + 1].wait_recv()
                x_f[kc + 1].start()
            for args in plan.get((kc, i0), ()):
                forward(*args)
            if (kc, i0) == (0, 0):
                from_source(in1, w2_pieces, not_up=2, not_down=1)
            if (kc, i0) == (1, 8):
                from_source(in1, w2_pieces, not_up=1, not_down=2)
            if (kc, i0) == (2, 8):
                h_out(jn).start()

    def down_rows(kk):
        k, h = kk * COL // BLK, kk * COL % BLK
        wait_slab_part(kk)
        for i in range(n_exp):
            vals = dot(hid[i], block(n_up + k * n_exp + i)[:, h:h + COL]).astype(BF16)
            rows = pl.ds(i * pair_rows, pair_rows)
            rk[0, kk % 3, rows, :] = vals[0:pair_rows]
            rk[1, kk % 3, rows, :] = vals[pair_rows:]

    def combine(p, kk, first, n):
        vals = rk[p, kk % 3]
        total = dot(gt[p, pl.ds(first, n)], vals)
        for m in range(1, 3):
            total += dot(gt[p, pl.ds(2 * m * n_tok + first, n)], vals)
        return total

    ret_p, ret_l, ret_y = [], [], []
    for kk in range(n_col):
        ret_p.append(rdma(racc.at[kk, 1 - c], precv.at[kk], ret_s.at[0], ret_r.at[0, kk], partner))
        ret_l.append(rdma(lacc.at[kk, 1 - c], lrecv.at[kk], ret_s.at[0], ret_r.at[1, kk], partner))
        ret_y.append(rdma(ysend.at[kk], yrecv.at[kk], ret_s.at[1], ret_r.at[2, kk], opp))

    def far_sum(kk):
        if kk == 0:
            for half in (1 - c, c):
                racc[kk, half] = combine(1, kk, pl.multiple_of(half * n_tok, n_tok), n_tok)
                if half is not c:
                    ret_p[kk].start()
        else:
            total = combine(1, kk, 0, 2 * n_tok)
            racc[kk, 0] = total[0:n_tok]
            racc[kk, 1] = total[n_tok:]
            ret_p[kk].start()

    def near_sum(kk):
        total = combine(0, kk, 0, 2 * n_tok)
        lacc[kk, 0] = total[0:n_tok]
        lacc[kk, 1] = total[n_tok:]

    down_rows(0)
    for kk in range(n_col):
        far_sum(kk)
        if kk > 0:
            near_sum(kk - 1)
        if kk + 1 < n_col:
            down_rows(kk + 1)
        ret_p[kk].wait_recv()
        ysend[kk] = racc[kk, c] + precv[kk]
        ret_y[kk].start()
        for args in plan.get(kk, ()):
            forward(*args)
        if kk == 3:
            need_far(0)
            need_far(1)
            h_far[jf] = shared_hidden(1, jf)
            h_out(jf).start()
    near_sum(n_col - 1)
    for j in range(2):
        h_near[2 * j + y] = shared_hidden(0, j)
    for j in range(2):
        h_out(j).wait_recv()
    for q in range(4):
        h_all[:, q * hid_w:(q + 1) * hid_w] = h_near[q]
    for kk in range(n_col):
        if kk * COL % BLK == 0:
            need_near(2 + kk * COL // BLK)
            need_far(2 + kk * COL // BLK)
        part = dot(h_all[...], ws2[:, kk * COL:(kk + 1) * COL])
        lacc[kk, 0] = lacc[kk, 0] + part[0:n_tok]
        lacc[kk, 1] = lacc[kk, 1] + part[n_tok:]
        ret_l[kk].start()

    for kk in range(n_col):
        ret_l[kk].wait_recv()
        ret_y[kk].wait_recv()
        cols = slice(kk * COL, (kk + 1) * COL)
        out[:, cols] = (x_all[0, my_rows, cols].astype(F32) + lacc[kk, c] + lrecv[kk] + yrecv[kk]).astype(BF16)

    def sent(ref, sem):
        pltpu.make_async_copy(ref, ref, sem).wait()

    for copy in [rt_p, rt_o, rt_f, x_p, h_out(0), h_out(1)]:
        copy.wait_send()
    sent(mine, xo_s)
    sent(mine, xf_s)
    sent(racc, ret_s.at[0])
    sent(ysend, ret_s.at[1])
    pieces = ws2.at[0:2 * hid_w, :]
    for j, s in ((jn, s_near), (jf, s_far)):
        @pl.when(s != z)
        def _():
            sent(pieces, xs_s.at[j])

        @pl.when(jnp.logical_and(z >= s, z < 3))
        def _():
            sent(pieces, zup_s.at[j])

        @pl.when(jnp.logical_and(z <= s, z > 0))
        def _():
            sent(pieces, zdn_s.at[j])


def solution(mesh):
    ep_size = mesh.shape["ep"]
    row_spec = P(("dp", "ep", "tp"), None)
    expert_spec = P("ep", None, None)

    def local_layer(tokens, expert_ids, gates, slots, sw1, sw3, sw2, ew1, ew3, ew2):
        n_tok, d_model = tokens.shape
        top_k = expert_ids.shape[1]
        n_exp, _, ff = ew1.shape
        cap = 8 * max(1, -(-2 * n_tok * top_k // (8 * n_exp * ep_size)))
        pair_rows = 2 * cap
        hid_w = sw1.shape[1] // 2
        n_blk, n_col = d_model // BLK, d_model // COL
        dma = pltpu.SemaphoreType.DMA
        vmem = pl.BlockSpec(memory_space=pltpu.VMEM)
        hbm = pl.BlockSpec(memory_space=pl.ANY)
        return pl.pallas_call(
            functools.partial(moe_kernel, cap),
            out_shape=pltpu.VMEM((n_tok, d_model), BF16),
            in_specs=[hbm] * 10,
            out_specs=vmem,
            scratch_shapes=[
                pltpu.VMEM((top_k, n_tok), jnp.int32), pltpu.VMEM((top_k, n_tok), F32), pltpu.VMEM((top_k, n_tok), jnp.int32),
                pltpu.VMEM((2, 16, 2 * n_tok), F32),
                pltpu.VMEM((2, 2 * n_tok, d_model), BF16),
                pltpu.VMEM((2, n_exp * pair_rows, 2 * n_tok), BF16),
                pltpu.VMEM((n_exp, 2 * pair_rows, d_model), BF16),
                pltpu.VMEM((n_exp, 2 * pair_rows, ff), F32),
                pltpu.VMEM((n_exp, 2 * pair_rows, ff), F32),
                pltpu.VMEM((n_exp, 2 * pair_rows, ff), BF16),
                pltpu.VMEM((RING, GROUP, BLK, ff), BF16),
                pltpu.VMEM((2, 6 * n_tok, n_exp * pair_rows), BF16),
                pltpu.VMEM((2, 3, n_exp * pair_rows, COL), BF16),
                pltpu.VMEM((2, d_model, hid_w), BF16),
                pltpu.VMEM((2, d_model, hid_w), BF16),
                pltpu.VMEM((4 * hid_w, d_model), BF16),
                pltpu.VMEM((2, 2 * n_tok, hid_w), BF16),
                pltpu.VMEM((4, 2 * n_tok, hid_w), BF16),
                pltpu.VMEM((2 * n_tok, 4 * hid_w), BF16),
                pltpu.VMEM((n_col, 2, n_tok, COL), F32),
                pltpu.VMEM((n_col, 2, n_tok, COL), F32),
                pltpu.VMEM((n_col, n_tok, COL), F32),
                pltpu.VMEM((n_col, n_tok, COL), F32),
                pltpu.VMEM((n_col, n_tok, COL), F32),
                pltpu.VMEM((n_col, n_tok, COL), F32),
                dma, dma((3,)), dma((RING,)), dma((n_col,)), dma((3,)), dma((4,)), dma((4,)),
                dma, dma((n_blk,)), dma, dma((n_blk,)),
                dma((2,)), dma((2,)), dma((2, 2 + n_blk)), dma((2,)), dma((2, 2 + n_blk)),
                dma((2,)), dma((3, n_col)), dma((2,)), dma((2,)),
            ],
            compiler_params=pltpu.CompilerParams(collective_id=0, has_side_effects=True, vmem_limit_bytes=66 * 1000 * 1000),
            name="moe_layer",
        )(expert_ids.T, gates.T, slots.T, tokens, sw1, sw3, sw2, ew1, ew3, ew2)

    return jax.shard_map(
        local_layer, mesh=mesh,
        in_specs=(row_spec, row_spec, row_spec, row_spec, P(None, "tp"), P(None, "tp"), P("tp", None), expert_spec, expert_spec, expert_spec),
        out_specs=row_spec, check_vma=False)
```
